32 devices in a mesh: gx: 8 (over z, y), gy: 2 (over x), ha: 2 (over core).
Axes of the slice: x: 2, y: 2, z: 4, core: 2. Of those that a mesh axis runs over, the one named last changes fastest.
Arguments:
- coupling: bfloat16 [8, 4, 4, 768, 768], P('gx', ('gy', 'ha')), may hold values from -0.125 to 0.125
- interior_inverse: bfloat16 [8, 4, 4, 768, 768], P('gx', ('gy', 'ha')), as said below
- boundary_stiffness: bfloat16 [8, 4, 768, 768], P('gx', ('gy', 'ha')), as said below
- block_counts: int32 [8, 4], P('gx', ('gy', 'ha')), may hold values from 1 to 4, as said below
- initial_traces: float32 [8, 4, 768, 128], P('gx', ('gy', 'ha')), may hold values from -2 to 2
- trace_loads: float32 [8, 4, 768, 128], P('gx', ('gy', 'ha')), may hold values from -18 to 18
Outputs:
- traces: float32 [8, 4, 768, 128], P('gx', ('gy', 'ha'))
- residual: float32 [8, 4, 768, 128], P('gx', ('gy', 'ha'))
The draws below stay inside these ranges and needn't reach their ends.
Inputs may be any that keep to these rules, and one draw needn't show every extreme that they name: `block_counts`: the two cells in columns 2m and 2m+1 of one grid row hold at most 5 blocks together; some cell holds 4. `interior_inverse`: symmetric in its last two dimensions. `boundary_stiffness`: symmetric in its last two dimensions.
All inputs are finite; a program needn't handle non-finite values.
Results may differ from the reference program's by a relative error of at most 0.00095.
Values may be sent and summed in bfloat16 or wider, within the bound.
A program may use at most 128 MiB of HBM per device.

```python
import jax
import jax.numpy as jnp
from jax import lax

MODES = 128
FACES = 6
TR = 768
INTR = 768
SLOTS = 4
LOADS = 128
SWEEPS = 3
NX = 8
NYC = 4


def symmetric_noise(key, shape, spread):
    noise = jnp.clip(jax.random.normal(key, shape, jnp.float32), -4.0, 4.0) * spread
    return (noise + jnp.swapaxes(noise, -1, -2)) / jnp.sqrt(2.0)


def draw_interior_inverse(key, part):
    key_noise = jax.random.fold_in(jax.random.fold_in(key, 11), 0)
    shape = (NX, NYC, SLOTS, INTR, INTR)
    symmetric = symmetric_noise(key_noise, shape, 0.25 / INTR ** 0.5)
    diagonal = jnp.ones(shape[:-1], jnp.float32)
    identity = jnp.eye(INTR, dtype=jnp.float32)
    return (symmetric + diagonal[..., None] * identity).astype(jnp.bfloat16)


def draw_boundary_stiffness(key, part):
    key_noise = jax.random.fold_in(jax.random.fold_in(key, 23), 0)
    shape = (NX, NYC, TR, TR)
    symmetric = symmetric_noise(key_noise, shape, 1.5 / TR ** 0.5)
    diagonal = jnp.full(shape[:-1], 7.0, jnp.float32)
    identity = jnp.eye(TR, dtype=jnp.float32)
    return (symmetric + diagonal[..., None] * identity).astype(jnp.bfloat16)


def draw_block_counts(key, part):
    key_first, key_second, key_flip = jax.random.split(jax.random.fold_in(key, 37), 3)
    pair_shape = (NX, NYC // 2)
    first_count = jax.random.randint(key_first, pair_shape, 1, 5)
    second_count = jax.random.randint(key_second, pair_shape, 1, 6 - first_count)
    flipped = jax.random.randint(key_flip, pair_shape, 0, 2)
    lower_cell = jnp.where(flipped == 1, second_count, first_count)
    upper_cell = jnp.where(flipped == 1, first_count, second_count)
    lower_cell = lower_cell.at[0, 0].set(4)
    upper_cell = upper_cell.at[0, 0].set(1)
    return jnp.stack([lower_cell, upper_cell], -1).reshape(NX, NYC).astype(jnp.int32)


def block_levels(rng, extent, shards, least, high):
    def one(position, blocks):
        heights = jax.random.uniform(jax.random.fold_in(jax.random.fold_in(rng, 6), position), (blocks,), jnp.float32, least / len(shards), high / len(shards))
        return jnp.repeat(jnp.exp(heights), extent[position] // blocks).reshape((-1,) + (1,) * (len(extent) - position - 1))

    level = one(*shards[0])
    for cut in shards[1:]:
        level = level * one(*cut)
    return level


def normal_values(own_key, extent, width, most, shards=(), kind=jnp.bfloat16):
    gain = block_levels(own_key, extent, shards, -0.22, 0.18) if shards else 1.0
    result = jax.random.normal(own_key, extent, jnp.float32) * width * gain
    return jnp.minimum(jnp.maximum(result, -most), most).astype(kind)


def setup_inputs(seed: int = 0) -> dict:
    seeds = jax.random.split(jax.random.key(seed), 7)
    coupling = normal_values(seeds[0], (NX, NYC, SLOTS, TR, INTR), (3 * INTR) ** -0.5, 0.125, ((0, 8), (1, 4)))
    interior_inverse = draw_interior_inverse(jax.random.fold_in(seeds[6], 71), 0)
    boundary_stiffness = draw_boundary_stiffness(jax.random.fold_in(seeds[6], 71), 0)
    block_counts = draw_block_counts(jax.random.fold_in(seeds[6], 71), 0)
    initial_traces = normal_values(seeds[4], (NX, NYC, TR, LOADS), 0.3, 2.0, ((0, 8), (1, 4)), jnp.float32)
    trace_loads = normal_values(seeds[5], (NX, NYC, TR, LOADS), 3.0, 18.0, ((0, 8), (1, 4)), jnp.float32)
    return {"coupling": coupling, "interior_inverse": interior_inverse, "boundary_stiffness": boundary_stiffness, "block_counts": block_counts, "initial_traces": initial_traces, "trace_loads": trace_loads}


penalty_weight = 2.0
lower_bound = 1.0
upper_bound = 14.0
spectrum_centre = (upper_bound + lower_bound) / 2.0
spectrum_half = (upper_bound - lower_bound) / 2.0
sigma_ratio = spectrum_centre / spectrum_half


def schur_block(coupling_block, inverse_block):
    product = jnp.dot(coupling_block, inverse_block, preferred_element_type=jnp.float32).astype(jnp.bfloat16)
    return jnp.dot(product, coupling_block.T, preferred_element_type=jnp.float32)


def condense_cell(packed):
    coupling, inverse, stiffness, blocks = packed
    condensed = stiffness.astype(jnp.float32)
    for slot_index in range(SLOTS):
        term = lax.cond(blocks > slot_index,
                        lambda: schur_block(coupling[slot_index], inverse[slot_index]),
                        lambda: jnp.zeros((TR, TR), jnp.float32))
        condensed = condensed - term
    return condensed


def apply_operator(condensed, traces):
    coupled = jnp.einsum("abij,abjl->abil", condensed, traces, precision=lax.Precision.HIGHEST)
    face_traces = traces.reshape(NX, NYC, FACES, MODES, LOADS)
    nothing_row = jnp.zeros((1, NYC, MODES, LOADS), jnp.float32)
    nothing_col = jnp.zeros((NX, 1, MODES, LOADS), jnp.float32)
    from_below_x = jnp.concatenate([nothing_row, face_traces[:-1, :, 1]], 0)
    from_above_x = jnp.concatenate([face_traces[1:, :, 0], nothing_row], 0)
    from_below_y = jnp.concatenate([nothing_col, face_traces[:, :-1, 3]], 1)
    from_above_y = jnp.concatenate([face_traces[:, 1:, 2], nothing_col], 1)
    absent = jnp.zeros_like(from_below_x)
    neighbours = jnp.stack([from_below_x, from_above_x, from_below_y, from_above_y, absent, absent], 2)
    neighbours = neighbours.reshape(NX, NYC, TR, LOADS)
    return coupled + penalty_weight * (traces - neighbours)


def reference(coupling, interior_inverse, boundary_stiffness, block_counts, initial_traces, trace_loads):
    cell_total = NX * NYC
    condensed = lax.map(condense_cell, (coupling.reshape(cell_total, SLOTS, TR, INTR),
                                        interior_inverse.reshape(cell_total, SLOTS, INTR, INTR),
                                        boundary_stiffness.reshape(cell_total, TR, TR),
                                        block_counts.reshape(cell_total)))
    condensed = condensed.reshape(NX, NYC, TR, TR)
    traces = initial_traces
    residual = trace_loads - apply_operator(condensed, traces)
    direction = residual / spectrum_centre
    weight_old = 1.0 / sigma_ratio
    for sweep_index in range(SWEEPS):
        traces = traces + direction
        residual = trace_loads - apply_operator(condensed, traces)
        if sweep_index + 1 < SWEEPS:
            weight_new = 1.0 / (2.0 * sigma_ratio - weight_old)
            direction = weight_new * weight_old * direction + (2.0 * weight_new / spectrum_half) * residual
            weight_old = weight_new
    return traces, residual
```

```python
import functools

import jax
import jax.numpy as jnp
from jax import lax
from jax.experimental import pallas as pl
from jax.experimental.pallas import tpu as pltpu
from jax.sharding import PartitionSpec as P

SWEEPS = 3
FACES = 6
LINKED = 4
BLOCK_FACES = 2

penalty_weight = 2.0
lower_bound = 1.0
upper_bound = 14.0
spectrum_centre = (upper_bound + lower_bound) / 2.0
spectrum_half = (upper_bound - lower_bound) / 2.0
sigma_ratio = spectrum_centre / spectrum_half

guess_slope = 8.0


def sweep_weights():
    weights = [(0.0, 1.0 / spectrum_centre)]
    weight_old = 1.0 / sigma_ratio
    for _ in range(SWEEPS - 1):
        weight_new = 1.0 / (2.0 * sigma_ratio - weight_old)
        weights.append((weight_new * weight_old, 2.0 * weight_new / spectrum_half))
        weight_old = weight_new
    return weights


def two_parts(value):
    high = value.astype(jnp.bfloat16)
    low = (value - high.astype(jnp.float32)).astype(jnp.bfloat16)
    return high, low


def dot_nn(left, right):
    return lax.dot_general(left, right, (((1,), (0,)), ((), ())), preferred_element_type=jnp.float32)


def dot_nt(left, right):
    return lax.dot_general(left, right, (((1,), (1,)), ((), ())), preferred_element_type=jnp.float32)


def kernel(
    axis_sizes,
    coupling,
    inverse,
    stiffness,
    counts,
    initial,
    loads,
    traces_out,
    residual_out,
    wide,
    inv,
    stiff,
    products,
    a_high,
    a_low,
    held,
    bound,
    parts,
    traces,
    bound_t,
    residual,
    direction,
    local,
    near,
    guess,
    sent,
    sent_half,
    landed,
    landed_half,
    in_sems,
    send_sems,
    recv_sems,
):
    slots, trace_width, inner_width = coupling.shape
    load_width = initial.shape[1]
    mode = trace_width // FACES
    block = BLOCK_FACES * mode
    blocks = trace_width // block
    rows, groups, halves = axis_sizes
    columns = groups * halves
    row = lax.axis_index("gx")
    column = lax.axis_index("gy") * halves + lax.axis_index("ha")

    def column_id(index):
        return {"gy": lax.div(index, halves), "ha": lax.rem(index, halves)}

    routes = (
        (0, 1, row > 0, {"gx": row - 1}),
        (1, 0, row + 1 < rows, {"gx": row + 1}),
        (2, 3, column > 0, column_id(column - 1)),
        (3, 2, column + 1 < columns, column_id(column + 1)),
    )

    first_copies = [
        pltpu.make_async_copy(initial, held, in_sems.at[0]),
        pltpu.make_async_copy(loads, bound, in_sems.at[1]),
    ]
    stiff_copy = pltpu.make_async_copy(stiffness, stiff, in_sems.at[2])

    def inner_span(slot):
        return pl.ds(slot * inner_width, inner_width)

    coupling_copies, inverse_copies = [], []
    for slot in range(slots):
        coupling_copies.append(
            pltpu.make_async_copy(coupling.at[slot], wide.at[:, inner_span(slot)], in_sems.at[3 + slot])
        )
        inverse_copies.append(
            pltpu.make_async_copy(inverse.at[slot], inv.at[slot], in_sems.at[3 + slots + slot])
        )
    coupling_copies[0].start()
    inverse_copies[0].start()
    for copy in first_copies:
        copy.start()
    for slot in range(1, slots):
        coupling_copies[slot].start()
        inverse_copies[slot].start()
    stiff_copy.start()

    barrier = pltpu.get_barrier_semaphore()
    partners = 0
    for _, _, exists, target in routes:
        partners = partners + exists.astype(jnp.int32)

        @pl.when(exists)
        def _():
            pl.semaphore_signal(barrier, inc=1, device_id=target, device_id_type=pl.DeviceIdType.MESH)

    for face, _, exists, _ in routes:

        @pl.when(jnp.logical_not(exists))
        def _():
            landed[:, face] = jnp.zeros((2, mode, load_width), jnp.float32)
            landed_half[:, face] = jnp.zeros((2, mode, load_width), jnp.bfloat16)

    def message(step, route, arriving=False):
        face, spot, _, target = route
        if arriving:
            spot = face
        source = (
            initial.at[pl.ds(face * mode, mode)],
            sent.at[face],
            sent_half.at[0, face],
            sent_half.at[1, face],
        )[step]
        place = landed.at[step, spot] if step < 2 else landed_half.at[step - 2, spot]
        return pltpu.make_async_remote_copy(
            src_ref=source,
            dst_ref=place,
            send_sem=send_sems.at[step, face],
            recv_sem=recv_sems.at[step, spot],
            device_id=target,
            device_id_type=pl.DeviceIdType.MESH,
        )

    def send(step, faces):
        for route in routes:
            if route[0] in faces:

                @pl.when(route[2])
                def _():
                    message(step, route).start()

    def wait_arrived(step):
        for route in routes:

            @pl.when(route[2])
            def _():
                message(step, route, True).wait_recv()

    def wait_sent():
        for step in range(SWEEPS + 1):
            for route in routes:

                @pl.when(route[2])
                def _():
                    message(step, route).wait_send()

    def there(face):
        return jnp.where(routes[face][2], 1.0, 0.0)

    def face_span(face):
        return pl.ds(face * mode, mode)

    def block_span(index):
        return pl.ds(index * block, block)

    def block_rows(index):
        return slice(index * block, (index + 1) * block)

    weights = sweep_weights()

    def products_of(index):
        span = block_span(index)
        for slot in range(slots):
            if index == 0:
                coupling_copies[slot].wait()
                inverse_copies[slot].wait()
            value = dot_nn(wide[span, inner_span(slot)], inv[slot])
            value = value * jnp.where(counts[0, 0] > slot, 1.0, 0.0)
            products[span, inner_span(slot)] = value.astype(jnp.bfloat16)

    def condense(index):
        span = block_span(index)
        for other in range(index, blocks):
            place = block_span(other)
            value = stiff[span, place].astype(jnp.float32) - dot_nt(products[span, :], wide[place, :])
            a_high[span, place], a_low[span, place] = two_parts(value)

    def applied(index):
        span = block_span(index)
        after = pl.ds(index * block, trace_width - index * block)
        both = dot_nt(parts[:, after], a_high[span, after])
        rest = dot_nt(parts[pl.ds(0, load_width), after], a_low[span, after])
        if index > 0:
            before = pl.ds(0, index * block)
            both = both + dot_nn(parts[:, before], a_high[before, span])
            rest = rest + dot_nn(parts[pl.ds(0, load_width), before], a_low[before, span])
        return both[:load_width] + both[load_width:] + rest

    def keep_parts(value):
        high, low = two_parts(value)
        parts[pl.ds(0, load_width)] = high
        parts[pl.ds(load_width, load_width)] = low

    for copy in first_copies:
        copy.wait()
    start = held[...].T
    traces[...] = start
    keep_parts(start)
    bound_t[...] = bound[...].T

    products_of(0)
    pl.semaphore_wait(barrier, partners)
    send(0, range(LINKED))
    stiff_copy.wait()

    for index in range(blocks):
        if index > 0:
            products_of(index)
        condense(index)
        span = block_span(index)
        value = bound_t[:, span] - applied(index) - penalty_weight * traces[:, span]
        local[:, span] = value
        faces = [face for face in range(LINKED) if face // BLOCK_FACES == index]
        for face in faces:
            sent[face] = value[:, (face % BLOCK_FACES) * mode : (face % BLOCK_FACES + 1) * mode]
        send(1, faces)

    wait_arrived(0)
    for face in range(FACES):
        span = face_span(face)
        value = local[:, span]
        if face < LINKED:
            value = value + penalty_weight * landed[0, face].T
        residual[:, span] = value
        change = weights[0][1] * value
        direction[:, span] = change
    keep_parts(direction[...])

    for index in range(blocks):
        span = block_span(index)
        value = residual[:, span] - applied(index) - penalty_weight * direction[:, span]
        local[:, span] = value
        faces = [face for face in range(LINKED) if face // BLOCK_FACES == index]
        for face in faces:
            sent_half[0, face] = value[
                :, (face % BLOCK_FACES) * mode : (face % BLOCK_FACES + 1) * mode
            ].astype(jnp.bfloat16)
        send(2, faces)

    wait_arrived(1)
    for face in range(FACES):
        span = face_span(face)
        value = local[:, span]
        own = traces[:, span]
        old = direction[:, span]
        if face < LINKED:
            beyond = (weights[0][1] * there(face)) * (landed[1, face] + penalty_weight * own)
            near[0, face] = beyond
            value = value + penalty_weight * beyond
            view = sent_half[0, face].astype(jnp.float32) + penalty_weight * beyond
            view_change = weights[1][0] * old + weights[1][1] * view
            guess[face] = view - guess_slope * view_change
        change = weights[1][0] * old + weights[1][1] * value
        residual[:, span] = value
        near[1, face] = change
        traces[:, span] = own + old + change
    for face in range(FACES):
        span = face_span(face)
        high, low = two_parts(near[1, face])
        parts[pl.ds(0, load_width), span] = high
        parts[pl.ds(load_width, load_width), span] = low

    for index in range(blocks):
        value = applied(index)
        for face in range(index * BLOCK_FACES, (index + 1) * BLOCK_FACES):
            span = face_span(face)
            lane = (face % BLOCK_FACES) * mode
            mine = residual[:, span] - value[:, lane : lane + mode] - penalty_weight * near[1, face]
            local[:, span] = mine
            if face < LINKED:
                sent_half[1, face] = (mine - guess[face]).astype(jnp.bfloat16)
        send(3, [face for face in range(LINKED) if face // BLOCK_FACES == index])

    wait_arrived(2)
    for face in range(FACES):
        span = face_span(face)
        value = local[:, span]
        old = near[1, face]
        if face < LINKED:
            view = landed_half[0, face].astype(jnp.float32) + penalty_weight * direction[:, span]
            beyond = there(face) * (weights[1][0] * near[0, face] + weights[1][1] * view)
            value = value + penalty_weight * beyond
            near[0, face] = beyond
            landed[1, face] = view - guess_slope * beyond + penalty_weight * old
        change = weights[2][0] * old + weights[2][1] * value
        residual[:, span] = value
        direction[:, span] = change
        traces[:, span] = traces[:, span] + change
    keep_parts(direction[...])

    for index in range(blocks):
        span = block_span(index)
        value = residual[:, span] - applied(index) - penalty_weight * direction[:, span]
        residual_out[span] = value.T
    traces_out[...] = traces[...].T

    wait_arrived(3)
    for face in range(LINKED):
        span = face_span(face)
        view = landed[1, face] + landed_half[1, face].astype(jnp.float32)
        beyond = weights[2][0] * near[0, face] + weights[2][1] * view
        beyond = (penalty_weight * there(face)) * beyond
        residual_out[span] = residual_out[span] + beyond.T
    wait_sent()


def write_kernel(traces, residual, traces_out, residual_out, sems):
    copies = [
        pltpu.make_async_copy(traces, traces_out, sems.at[0]),
        pltpu.make_async_copy(residual, residual_out, sems.at[1]),
    ]
    for copy in copies:
        copy.start()
    for copy in copies:
        copy.wait()


def in_hbm(value):
    return pltpu.with_memory_space_constraint(value, pltpu.HBM)


def on_device(
    axis_sizes, coupling, interior_inverse, boundary_stiffness, block_counts, initial_traces, trace_loads
):
    slots, trace_width, inner_width = coupling.shape[2:]
    load_width = initial_traces.shape[-1]
    mode = trace_width // FACES
    whole = pl.BlockSpec(memory_space=pltpu.HBM)
    vmem = pl.BlockSpec(memory_space=pltpu.VMEM)
    out = pltpu.VMEM((trace_width, load_width), jnp.float32)
    tall = pltpu.VMEM((trace_width, load_width), jnp.float32)
    flat = pltpu.VMEM((load_width, trace_width), jnp.float32)
    square = pltpu.VMEM((trace_width, trace_width), jnp.bfloat16)
    long = pltpu.VMEM((trace_width, slots * inner_width), jnp.bfloat16)
    traces, residual = pl.pallas_call(
        functools.partial(kernel, axis_sizes),
        out_shape=(out, out),
        in_specs=[whole, whole, whole, pl.BlockSpec(memory_space=pltpu.SMEM), whole, whole],
        out_specs=(vmem, vmem),
        scratch_shapes=[
            long,
            pltpu.VMEM((slots, inner_width, inner_width), jnp.bfloat16),
            square,
            long,
            square,
            square,
            tall,
            tall,
            pltpu.VMEM((2 * load_width, trace_width), jnp.bfloat16),
            flat,
            flat,
            flat,
            flat,
            flat,
            pltpu.VMEM((2, FACES, load_width, mode), jnp.float32),
            pltpu.VMEM((LINKED, load_width, mode), jnp.float32),
            pltpu.VMEM((LINKED, load_width, mode), jnp.float32),
            pltpu.VMEM((2, LINKED, load_width, mode), jnp.bfloat16),
            pltpu.VMEM((2, LINKED, load_width, mode), jnp.float32),
            pltpu.VMEM((2, LINKED, load_width, mode), jnp.bfloat16),
            pltpu.SemaphoreType.DMA((3 + 2 * slots,)),
            pltpu.SemaphoreType.DMA((SWEEPS + 1, LINKED)),
            pltpu.SemaphoreType.DMA((SWEEPS + 1, LINKED)),
        ],
        compiler_params=pltpu.CompilerParams(
            collective_id=0, has_side_effects=True, vmem_limit_bytes=48 << 20
        ),
        name="condense_and_sweep",
    )(
        in_hbm(coupling[0, 0]),
        in_hbm(interior_inverse[0, 0]),
        in_hbm(boundary_stiffness[0, 0]),
        block_counts,
        in_hbm(initial_traces[0, 0]),
        in_hbm(trace_loads[0, 0]),
    )
    result = jax.ShapeDtypeStruct((trace_width, load_width), jnp.float32)
    traces, residual = pl.pallas_call(
        write_kernel,
        out_shape=(result, result),
        in_specs=[vmem, vmem],
        out_specs=(whole, whole),
        scratch_shapes=[pltpu.SemaphoreType.DMA((2,))],
        name="write_results",
    )(
        pltpu.with_memory_space_constraint(traces, pltpu.VMEM),
        pltpu.with_memory_space_constraint(residual, pltpu.VMEM),
    )
    return (traces[None, None], residual[None, None])


def solution(mesh):
    in_specs = (
        P("gx", ("gy", "ha"), None, None, None),
        P("gx", ("gy", "ha"), None, None, None),
        P("gx", ("gy", "ha"), None, None),
        P("gx", ("gy", "ha")),
        P("gx", ("gy", "ha"), None, None),
        P("gx", ("gy", "ha"), None, None),
    )
    out_specs = (P("gx", ("gy", "ha"), None, None), P("gx", ("gy", "ha"), None, None))
    axis_sizes = (mesh.shape["gx"], mesh.shape["gy"], mesh.shape["ha"])
    return jax.shard_map(
        functools.partial(on_device, axis_sizes),
        mesh=mesh, in_specs=in_specs, out_specs=out_specs, check_vma=False,
    )
```

```python
import functools

import jax
import jax.numpy as jnp
from jax import lax
from jax.experimental import pallas as pl
from jax.experimental.pallas import tpu as pltpu
from jax.sharding import PartitionSpec as P

SWEEPS = 3
FACES = 6
LINKED = 4
BLOCK_FACES = 2

penalty_weight = 2.0
lower_bound = 1.0
upper_bound = 14.0
spectrum_centre = (upper_bound + lower_bound) / 2.0
spectrum_half = (upper_bound - lower_bound) / 2.0
sigma_ratio = spectrum_centre / spectrum_half

guess_slope = 8.0


def sweep_weights():
    weights = [(0.0, 1.0 / spectrum_centre)]
    weight_old = 1.0 / sigma_ratio
    for _ in range(SWEEPS - 1):
        weight_new = 1.0 / (2.0 * sigma_ratio - weight_old)
        weights.append((weight_new * weight_old, 2.0 * weight_new / spectrum_half))
        weight_old = weight_new
    return weights


def two_parts(value):
    high = value.astype(jnp.bfloat16)
    low = (value - high.astype(jnp.float32)).astype(jnp.bfloat16)
    return high, low


def dot_nn(left, right):
    return lax.dot_general(left, right, (((1,), (0,)), ((), ())), preferred_element_type=jnp.float32)


def dot_nt(left, right):
    return lax.dot_general(left, right, (((1,), (1,)), ((), ())), preferred_element_type=jnp.float32)


def kernel(
    axis_sizes,
    coupling,
    inverse,
    stiffness,
    counts,
    initial,
    loads,
    traces_out,
    residual_out,
    wide,
    inv,
    stiff,
    products,
    a_high,
    a_low,
    given,
    parts,
    traces,
    bound_t,
    residual,
    direction,
    local,
    near,
    guess,
    sent,
    sent_half,
    landed,
    landed_half,
    total,
    in_sems,
    send_sems,
    recv_sems,
):
    slots, trace_width, inner_width = coupling.shape
    load_width = initial.shape[1]
    mode = trace_width // FACES
    block = BLOCK_FACES * mode
    blocks = trace_width // block
    rows, groups, halves = axis_sizes
    columns = groups * halves
    row = lax.axis_index("gx")
    column = lax.axis_index("gy") * halves + lax.axis_index("ha")

    def column_id(index):
        return {"gy": lax.div(index, halves), "ha": lax.rem(index, halves)}

    routes = (
        (0, 1, row > 0, {"gx": row - 1}),
        (1, 0, row + 1 < rows, {"gx": row + 1}),
        (2, 3, column > 0, column_id(column - 1)),
        (3, 2, column + 1 < columns, column_id(column + 1)),
    )

    def inner_span(slot):
        return pl.ds(slot * inner_width, inner_width)

    given_sem, slot_sem = in_sems.at[slots], in_sems
    pltpu.make_async_copy(initial, given.at[0], given_sem).start()
    pltpu.make_async_copy(loads, given.at[1], given_sem).start()
    for slot in range(slots):
        pltpu.make_async_copy(coupling.at[slot], wide.at[:, inner_span(slot)], slot_sem.at[slot]).start()
        pltpu.make_async_copy(inverse.at[slot], inv.at[slot], slot_sem.at[slot]).start()
    stiff_copy = pltpu.make_async_copy(stiffness, stiff, in_sems.at[slots + 1])
    stiff_copy.start()

    def wait_given():
        pltpu.make_async_copy(given, given, given_sem).wait()

    def wait_slot(slot):
        both = inv.at[pl.ds(0, 2)]
        pltpu.make_async_copy(both, both, slot_sem.at[slot]).wait()

    barrier = pltpu.get_barrier_semaphore()
    partners = 0
    for _, _, exists, target in routes:
        partners = partners + exists.astype(jnp.int32)

        @pl.when(exists)
        def _():
            pl.semaphore_signal(barrier, inc=1, device_id=target, device_id_type=pl.DeviceIdType.MESH)

    for face, _, exists, _ in routes:

        @pl.when(jnp.logical_not(exists))
        def _():
            landed[:, face] = jnp.zeros((2, mode, load_width), jnp.float32)
            landed_half[:, face] = jnp.zeros((2, mode, load_width), jnp.bfloat16)

    def message(step, route):
        face, spot, _, target = route
        source = (
            initial.at[pl.ds(face * mode, mode)],
            sent.at[face],
            sent_half.at[0, face],
            sent_half.at[1, face],
        )[step]
        place = landed.at[step, spot] if step < 2 else landed_half.at[step - 2, spot]
        return pltpu.make_async_remote_copy(
            src_ref=source,
            dst_ref=place,
            send_sem=send_sems.at[0],
            recv_sem=recv_sems.at[step],
            device_id=target,
            device_id_type=pl.DeviceIdType.MESH,
        )

    def send(step, faces):
        for route in routes:
            if route[0] in faces:

                @pl.when(route[2])
                def _():
                    message(step, route).start()

    def wait_bytes(place, per_face, sem):
        for number in range(1, LINKED + 1):

            @pl.when(partners == number)
            def _():
                part = place.at[pl.ds(0, number * per_face)]
                pltpu.make_async_copy(part, part, sem).wait()

    def wait_arrived(step):
        place = landed.at[step] if step < 2 else landed_half.at[step - 2]
        wait_bytes(place, 1, recv_sems.at[step])

    def wait_sent():
        wait_bytes(near, 3, send_sems.at[0])

    def there(face):
        return jnp.where(routes[face][2], 1.0, 0.0)

    def face_span(face):
        return pl.ds(face * mode, mode)

    def block_span(index):
        return pl.ds(index * block, block)

    def block_rows(index):
        return slice(index * block, (index + 1) * block)

    weights = sweep_weights()

    def product_of(index, slot):
        span = block_span(index)
        value = dot_nn(wide[span, inner_span(slot)], inv[slot])
        value = value * jnp.where(counts[0, 0] > slot, 1.0, 0.0)
        products[span, inner_span(slot)] = value.astype(jnp.bfloat16)

    def keep_condensed(index, other, value):
        span, place = block_span(index), block_span(other)
        value = stiff[span, place].astype(jnp.float32) - value
        a_high[span, place], a_low[span, place] = two_parts(value)

    def condense_first(slot):
        for other in range(blocks):
            place = block_span(other)
            value = dot_nt(products[block_span(0), inner_span(slot)], wide[place, inner_span(slot)])
            if slot > 0:
                value = value + total[:, place]
            if slot + 1 < slots:
                total[:, place] = value
            else:
                keep_condensed(0, other, value)

    def condense(index):
        for other in range(index, blocks):
            keep_condensed(index, other, dot_nt(products[block_span(index), :], wide[block_span(other), :]))

    def applied(index):
        span = block_span(index)
        after = pl.ds(index * block, trace_width - index * block)
        both = dot_nt(parts[:, after], a_high[span, after])
        rest = dot_nt(parts[pl.ds(0, load_width), after], a_low[span, after])
        if index > 0:
            before = pl.ds(0, index * block)
            both = both + dot_nn(parts[:, before], a_high[before, span])
            rest = rest + dot_nn(parts[pl.ds(0, load_width), before], a_low[before, span])
        return both[:load_width] + both[load_width:] + rest

    def keep_parts(value):
        high, low = two_parts(value)
        parts[pl.ds(0, load_width)] = high
        parts[pl.ds(load_width, load_width)] = low

    wait_given()
    start = given[0].T
    traces[...] = start
    keep_parts(start)
    bound_t[...] = given[1].T

    for slot in range(slots):
        wait_slot(slot)
        product_of(0, slot)
        if slot + 1 < slots:
            product_of(1, slot)
        if slot < 1:
            product_of(2, slot)
        if slot == 1:
            pl.semaphore_wait(barrier, partners)
            send(0, range(LINKED))
        if slot + 1 == slots:
            stiff_copy.wait()
        condense_first(slot)
    product_of(1, slots - 1)

    for index in range(blocks):
        if index > 1:
            for slot in range(1, slots):
                product_of(index, slot)
        if index > 0:
            condense(index)
        span = block_span(index)
        value = bound_t[:, span] - applied(index) - penalty_weight * traces[:, span]
        local[:, span] = value
        faces = [face for face in range(LINKED) if face // BLOCK_FACES == index]
        for face in faces:
            sent[face] = value[:, (face % BLOCK_FACES) * mode : (face % BLOCK_FACES + 1) * mode]
        send(1, faces)

    wait_arrived(0)
    for face in range(FACES):
        span = face_span(face)
        value = local[:, span]
        if face < LINKED:
            value = value + penalty_weight * landed[0, face].T
        residual[:, span] = value
        change = weights[0][1] * value
        direction[:, span] = change
    keep_parts(direction[...])

    for index in range(blocks):
        span = block_span(index)
        value = residual[:, span] - applied(index) - penalty_weight * direction[:, span]
        local[:, span] = value
        faces = [face for face in range(LINKED) if face // BLOCK_FACES == index]
        for face in faces:
            sent_half[0, face] = value[
                :, (face % BLOCK_FACES) * mode : (face % BLOCK_FACES + 1) * mode
            ].astype(jnp.bfloat16)
        send(2, faces)

    wait_arrived(1)
    for face in range(FACES):
        span = face_span(face)
        value = local[:, span]
        own = traces[:, span]
        old = direction[:, span]
        if face < LINKED:
            beyond = (weights[0][1] * there(face)) * (landed[1, face] + penalty_weight * own)
            near[face] = beyond
            value = value + penalty_weight * beyond
            view = sent_half[0, face].astype(jnp.float32) + penalty_weight * beyond
            view_change = weights[1][0] * old + weights[1][1] * view
            guess[face] = view - guess_slope * view_change
        change = weights[1][0] * old + weights[1][1] * value
        residual[:, span] = value
        near[FACES + face] = change
        traces[:, span] = own + old + change
    for face in range(FACES):
        span = face_span(face)
        high, low = two_parts(near[FACES + face])
        parts[pl.ds(0, load_width), span] = high
        parts[pl.ds(load_width, load_width), span] = low

    for index in range(blocks):
        value = applied(index)
        for face in range(index * BLOCK_FACES, (index + 1) * BLOCK_FACES):
            span = face_span(face)
            lane = (face % BLOCK_FACES) * mode
            mine = residual[:, span] - value[:, lane : lane + mode] - penalty_weight * near[FACES + face]
            local[:, span] = mine
            if face < LINKED:
                sent_half[1, face] = (mine - guess[face]).astype(jnp.bfloat16)
        send(3, [face for face in range(LINKED) if face // BLOCK_FACES == index])

    wait_arrived(2)
    for face in range(FACES):
        span = face_span(face)
        value = local[:, span]
        old = near[FACES + face]
        if face < LINKED:
            view = landed_half[0, face].astype(jnp.float32) + penalty_weight * direction[:, span]
            beyond = there(face) * (weights[1][0] * near[face] + weights[1][1] * view)
            value = value + penalty_weight * beyond
            near[face] = beyond
            landed[1, face] = view - guess_slope * beyond + penalty_weight * old
        change = weights[2][0] * old + weights[2][1] * value
        residual[:, span] = value
        direction[:, span] = change
        traces[:, span] = traces[:, span] + change
    keep_parts(direction[...])

    for index in range(blocks):
        span = block_span(index)
        value = residual[:, span] - applied(index) - penalty_weight * direction[:, span]
        residual_out[span] = value.T
    traces_out[...] = traces[...].T

    wait_sent()
    wait_arrived(3)
    for face in range(LINKED):
        span = face_span(face)
        view = landed[1, face] + landed_half[1, face].astype(jnp.float32)
        beyond = weights[2][0] * near[face] + weights[2][1] * view
        beyond = (penalty_weight * there(face)) * beyond
        residual_out[span] = residual_out[span] + beyond.T


def write_kernel(traces, residual, traces_out, residual_out, sems):
    copies = [
        pltpu.make_async_copy(traces, traces_out, sems.at[0]),
        pltpu.make_async_copy(residual, residual_out, sems.at[1]),
    ]
    for copy in copies:
        copy.start()
    for copy in copies:
        copy.wait()


def in_hbm(value):
    return pltpu.with_memory_space_constraint(value, pltpu.HBM)


def on_device(
    axis_sizes, coupling, interior_inverse, boundary_stiffness, block_counts, initial_traces, trace_loads
):
    slots, trace_width, inner_width = coupling.shape[2:]
    load_width = initial_traces.shape[-1]
    mode = trace_width // FACES
    whole = pl.BlockSpec(memory_space=pltpu.HBM)
    vmem = pl.BlockSpec(memory_space=pltpu.VMEM)
    out = pltpu.VMEM((trace_width, load_width), jnp.float32)
    flat = pltpu.VMEM((load_width, trace_width), jnp.float32)
    square = pltpu.VMEM((trace_width, trace_width), jnp.bfloat16)
    long = pltpu.VMEM((trace_width, slots * inner_width), jnp.bfloat16)
    traces, residual = pl.pallas_call(
        functools.partial(kernel, axis_sizes),
        out_shape=(out, out),
        in_specs=[whole, whole, whole, pl.BlockSpec(memory_space=pltpu.SMEM), whole, whole],
        out_specs=(vmem, vmem),
        scratch_shapes=[
            long,
            pltpu.VMEM((slots, inner_width, inner_width), jnp.bfloat16),
            square,
            long,
            square,
            square,
            pltpu.VMEM((2, trace_width, load_width), jnp.float32),
            pltpu.VMEM((2 * load_width, trace_width), jnp.bfloat16),
            flat,
            flat,
            flat,
            flat,
            flat,
            pltpu.VMEM((2 * FACES, load_width, mode), jnp.float32),
            pltpu.VMEM((LINKED, load_width, mode), jnp.float32),
            pltpu.VMEM((LINKED, load_width, mode), jnp.float32),
            pltpu.VMEM((2, LINKED, load_width, mode), jnp.bfloat16),
            pltpu.VMEM((2, LINKED, load_width, mode), jnp.float32),
            pltpu.VMEM((2, LINKED, load_width, mode), jnp.bfloat16),
            pltpu.VMEM((BLOCK_FACES * mode, trace_width), jnp.float32),
            pltpu.SemaphoreType.DMA((slots + 2,)),
            pltpu.SemaphoreType.DMA((1,)),
            pltpu.SemaphoreType.DMA((SWEEPS + 1,)),
        ],
        compiler_params=pltpu.CompilerParams(
            collective_id=0, has_side_effects=True, vmem_limit_bytes=48 << 20
        ),
        name="condense_and_sweep",
    )(
        in_hbm(coupling[0, 0]),
        in_hbm(interior_inverse[0, 0]),
        in_hbm(boundary_stiffness[0, 0]),
        block_counts,
        in_hbm(initial_traces[0, 0]),
        in_hbm(trace_loads[0, 0]),
    )
    result = jax.ShapeDtypeStruct((trace_width, load_width), jnp.float32)
    traces, residual = pl.pallas_call(
        write_kernel,
        out_shape=(result, result),
        in_specs=[vmem, vmem],
        out_specs=(whole, whole),
        scratch_shapes=[pltpu.SemaphoreType.DMA((2,))],
        name="write_results",
    )(
        pltpu.with_memory_space_constraint(traces, pltpu.VMEM),
        pltpu.with_memory_space_constraint(residual, pltpu.VMEM),
    )
    return (traces[None, None], residual[None, None])


def solution(mesh):
    in_specs = (
        P("gx", ("gy", "ha"), None, None, None),
        P("gx", ("gy", "ha"), None, None, None),
        P("gx", ("gy", "ha"), None, None),
        P("gx", ("gy", "ha")),
        P("gx", ("gy", "ha"), None, None),
        P("gx", ("gy", "ha"), None, None),
    )
    out_specs = (P("gx", ("gy", "ha"), None, None), P("gx", ("gy", "ha"), None, None))
    axis_sizes = (mesh.shape["gx"], mesh.shape["gy"], mesh.shape["ha"])
    return jax.shard_map(
        functools.partial(on_device, axis_sizes),
        mesh=mesh, in_specs=in_specs, out_specs=out_specs, check_vma=False,
    )
```

```python
import functools

import jax
import jax.numpy as jnp
from jax import lax
from jax.experimental import pallas as pl
from jax.experimental.pallas import tpu as pltpu
from jax.sharding import PartitionSpec as P

SWEEPS = 3
FACES = 6
LINKED = 4
BLOCK_FACES = 2
EARLY = 2
MEET = 0
NW = 256

penalty_weight = 2.0
lower_bound = 1.0
upper_bound = 14.0
spectrum_centre = (upper_bound + lower_bound) / 2.0
spectrum_half = (upper_bound - lower_bound) / 2.0
sigma_ratio = spectrum_centre / spectrum_half

guess_slope = 8.0


def sweep_weights():
    weights = [(0.0, 1.0 / spectrum_centre)]
    weight_old = 1.0 / sigma_ratio
    for _ in range(SWEEPS - 1):
        weight_new = 1.0 / (2.0 * sigma_ratio - weight_old)
        weights.append((weight_new * weight_old, 2.0 * weight_new / spectrum_half))
        weight_old = weight_new
    return weights


def two_parts(value):
    high = value.astype(jnp.bfloat16)
    low = (value - high.astype(jnp.float32)).astype(jnp.bfloat16)
    return high, low


def dot_nn(left, right):
    return lax.dot_general(left, right, (((1,), (0,)), ((), ())), preferred_element_type=jnp.float32)


def dot_nt(left, right):
    return lax.dot_general(left, right, (((1,), (1,)), ((), ())), preferred_element_type=jnp.float32)


def kernel(
    axis_sizes,
    coupling,
    inverse,
    stiffness,
    counts,
    initial,
    loads,
    traces_out,
    residual_out,
    wide,
    inv,
    stiff,
    products,
    a_high,
    a_low,
    given,
    parts,
    more_parts,
    traces,
    bound_t,
    residual,
    direction,
    local,
    near,
    sent,
    sent_half,
    landed,
    landed_half,
    total,
    in_sems,
    send_sems,
    recv_sems,
):
    slots, trace_width, inner_width = coupling.shape
    load_width = initial.shape[1]
    mode = trace_width // FACES
    block = BLOCK_FACES * mode
    blocks = trace_width // block
    rows, groups, halves = axis_sizes
    columns = groups * halves
    row = lax.axis_index("gx")
    column = lax.axis_index("gy") * halves + lax.axis_index("ha")

    def column_id(index):
        return {"gy": lax.div(index, halves), "ha": lax.rem(index, halves)}

    routes = (
        (0, 1, row > 0, {"gx": row - 1}),
        (1, 0, row + 1 < rows, {"gx": row + 1}),
        (2, 3, column > 0, column_id(column - 1)),
        (3, 2, column + 1 < columns, column_id(column + 1)),
    )

    def inner_span(slot):
        return pl.ds(slot * inner_width, inner_width)

    def coupling_copy(slot, start, size, sem):
        rows_of = pl.ds(start, size)
        pltpu.make_async_copy(coupling.at[slot, rows_of], wide.at[rows_of, inner_span(slot)], sem).start()

    def wait_for(place, sem):
        pltpu.make_async_copy(place, place, sem).wait()

    chunks = inner_width // block
    given_sem = in_sems.at[0]
    chunk_sems = [in_sems.at[1 + chunk] for chunk in range(chunks)]
    rest_sem, stiff_sem = in_sems.at[1 + chunks], in_sems.at[2 + chunks]
    slot_sems = [None] + [in_sems.at[2 + chunks + slot] for slot in range(1, slots)]
    coupling_copy(0, 0, block, chunk_sems[0])
    for chunk in range(chunks):
        piece = inv.at[0, pl.ds(chunk * block, block)]
        pltpu.make_async_copy(inverse.at[0, pl.ds(chunk * block, block)], piece, chunk_sems[chunk]).start()
    coupling_copy(0, block, trace_width - block, rest_sem)
    pltpu.make_async_copy(initial, given.at[0], given_sem).start()
    pltpu.make_async_copy(loads, given.at[1], given_sem).start()
    def load_slot(slot):
        coupling_copy(slot, 0, trace_width, slot_sems[slot])
        pltpu.make_async_copy(inverse.at[slot], inv.at[slot], slot_sems[slot]).start()

    def load_stiff():
        pltpu.make_async_copy(stiffness, stiff, stiff_sem).start()

    load_slot(1)

    def wait_slot(slot):
        wait_for(inv.at[pl.ds(0, 2)], slot_sems[slot])

    barrier = pltpu.get_barrier_semaphore()
    partners = 0
    for _, _, exists, target in routes:
        partners = partners + exists.astype(jnp.int32)

        @pl.when(exists)
        def _():
            pl.semaphore_signal(barrier, inc=1, device_id=target, device_id_type=pl.DeviceIdType.MESH)

    for face, _, exists, _ in routes:

        @pl.when(jnp.logical_not(exists))
        def _():
            landed[:, face] = jnp.zeros((2, mode, load_width), jnp.float32)
            landed_half[:, face] = jnp.zeros((2, mode, load_width), jnp.bfloat16)

    def message(step, route):
        face, spot, _, target = route
        source = (
            initial.at[pl.ds(face * mode, mode)],
            sent.at[face],
            sent_half.at[0, face],
            sent_half.at[1, face],
        )[step]
        place = landed.at[step, spot] if step < 2 else landed_half.at[step - 2, spot]
        return pltpu.make_async_remote_copy(
            src_ref=source,
            dst_ref=place,
            send_sem=send_sems.at[0],
            recv_sem=recv_sems.at[step],
            device_id=target,
            device_id_type=pl.DeviceIdType.MESH,
        )

    def send(step, faces):
        for route in routes:
            if route[0] in faces:

                @pl.when(route[2])
                def _():
                    message(step, route).start()

    def wait_bytes(place, per_face, sem):
        for number in range(1, LINKED + 1):

            @pl.when(partners == number)
            def _():
                part = place.at[pl.ds(0, number * per_face)]
                pltpu.make_async_copy(part, part, sem).wait()

    def wait_arrived(step):
        place = landed.at[step] if step < 2 else landed_half.at[step - 2]
        wait_bytes(place, 1, recv_sems.at[step])

    def wait_sent():
        wait_bytes(near, 3, send_sems.at[0])

    def there(face):
        return jnp.where(routes[face][2], 1.0, 0.0)

    def face_span(face):
        return pl.ds(face * mode, mode)

    def block_span(index):
        return pl.ds(index * block, block)

    def block_rows(index):
        return slice(index * block, (index + 1) * block)

    weights = sweep_weights()

    def product_of(index, slot):
        span = block_span(index)
        if index == 0 and slot == 0:
            value = 0.0
            for chunk in range(chunks):
                wait_for(inv.at[0, pl.ds(0, block * (2 if chunk == 0 else 1))], chunk_sems[chunk])
                if chunk == 0:
                    load_slot(2)
                inside = pl.ds(chunk * block, block)
                value = value + dot_nn(wide[span, inside], inv[slot, inside])
        else:
            live = jnp.where(counts[0, 0] > slot, 1.0, 0.0)
            for piece in range(inner_width // NW):
                inside = pl.ds(piece * NW, NW)
                value = dot_nn(wide[span, inner_span(slot)], inv[slot, :, inside]) * live
                products[span, pl.ds(slot * inner_width + piece * NW, NW)] = value.astype(jnp.bfloat16)
            return
        value = value * jnp.where(counts[0, 0] > slot, 1.0, 0.0)
        products[span, inner_span(slot)] = value.astype(jnp.bfloat16)

    def keep_condensed(index, other, value):
        span, place = block_span(index), block_span(other)
        value = stiff[span, place].astype(jnp.float32) - value
        a_high[span, place], a_low[span, place] = two_parts(value)

    def condense_first(slot):
        for other in range(blocks):
            place = block_span(other)
            value = dot_nt(products[block_span(0), inner_span(slot)], wide[place, inner_span(slot)])
            if slot > 0:
                value = value + total[:, place]
            if slot + 1 < slots:
                total[:, place] = value
            else:
                keep_condensed(0, other, value)

    def condense(index):
        for other in range(index, blocks):
            keep_condensed(index, other, dot_nt(products[block_span(index), :], wide[block_span(other), :]))

    def applied(index, source, depth):
        span = block_span(index)
        ones = pl.ds(0, load_width)
        both, rest = [], []
        if index < depth:
            after = pl.ds(index * block, (depth - index) * block)
            both.append(dot_nt(source[:, after], a_high[span, after]))
            rest.append(dot_nt(source[ones, after], a_low[span, after]))
        if index > 0:
            before = pl.ds(0, min(index, depth) * block)
            both.append(dot_nn(source[:, before], a_high[before, span]))
            rest.append(dot_nn(source[ones, before], a_low[before, span]))
        both, rest = sum(both[1:], both[0]), sum(rest[1:], rest[0])
        return both[:load_width] + both[load_width:] + rest

    def keep_face_parts(place, span, value):
        high, low = two_parts(value)
        place[pl.ds(0, load_width), span] = high
        place[pl.ds(load_width, load_width), span] = low

    def keep_parts(value):
        high, low = two_parts(value)
        parts[pl.ds(0, load_width)] = high
        parts[pl.ds(load_width, load_width)] = low

    for slot in range(slots):
        if slot > 0:
            wait_slot(slot)
        product_of(0, slot)
        if slot == 0:
            wait_for(wide.at[pl.ds(0, trace_width - block), inner_span(0)], rest_sem)
            load_slot(3)
            load_stiff()
        if slot < EARLY:
            product_of(1, slot)
        if slot == 0:
            wait_for(given, given_sem)
            start = given[0].T
            traces[...] = start
            keep_parts(start)
            bound_t[...] = given[1].T
        if slot == MEET:
            pl.semaphore_wait(barrier, partners)
            send(0, range(LINKED))
        if slot + 1 == slots:
            wait_for(stiff, stiff_sem)
        condense_first(slot)

    linked_blocks = LINKED // BLOCK_FACES
    for index in range(blocks):
        if index > 0:
            for slot in range(EARLY if index == 1 else 0, slots):
                product_of(index, slot)
            condense(index)
        span = block_span(index)
        value = bound_t[:, span] - applied(index, parts, blocks) - penalty_weight * traces[:, span]
        if index < linked_blocks:
            local[:, span] = value
            faces = range(index * BLOCK_FACES, (index + 1) * BLOCK_FACES)
            for face in faces:
                sent[face] = value[:, (face % BLOCK_FACES) * mode : (face % BLOCK_FACES + 1) * mode]
            send(1, faces)
        else:
            residual[:, span] = value
            change = weights[0][1] * value
            direction[:, span] = change
            keep_face_parts(more_parts, span, change)
        if index + 1 == linked_blocks:
            wait_arrived(0)
            for face in range(LINKED):
                span = face_span(face)
                value = local[:, span] + penalty_weight * landed[0, face].T
                residual[:, span] = value
                change = weights[0][1] * value
                direction[:, span] = change
                keep_face_parts(more_parts, span, change)

    for index in range(blocks):
        span = block_span(index)
        value = residual[:, span] - applied(index, more_parts, blocks) - penalty_weight * direction[:, span]
        local[:, span] = value
        faces = [face for face in range(LINKED) if face // BLOCK_FACES == index]
        for face in faces:
            sent_half[0, face] = value[
                :, (face % BLOCK_FACES) * mode : (face % BLOCK_FACES + 1) * mode
            ].astype(jnp.bfloat16)
        send(2, faces)

    wait_arrived(1)
    for face in range(FACES):
        span = face_span(face)
        value = local[:, span]
        if face < LINKED:
            beyond = (weights[0][1] * there(face)) * (landed[1, face] + penalty_weight * traces[:, span])
            near[face] = beyond
            value = value + penalty_weight * beyond
        change = weights[1][0] * direction[:, span] + weights[1][1] * value
        residual[:, span] = value
        near[FACES + face] = change
        keep_face_parts(parts, span, change)

    for index in range(blocks):
        value = applied(index, parts, blocks)
        for face in range(index * BLOCK_FACES, (index + 1) * BLOCK_FACES):
            span = face_span(face)
            lane = (face % BLOCK_FACES) * mode
            mine = residual[:, span] - value[:, lane : lane + mode] - penalty_weight * near[FACES + face]
            local[:, span] = mine
            if face < LINKED:
                view = sent_half[0, face].astype(jnp.float32) + penalty_weight * near[face]
                view_change = weights[1][0] * direction[:, span] + weights[1][1] * view
                sent_half[1, face] = (mine - (view - guess_slope * view_change)).astype(jnp.bfloat16)
        send(3, [face for face in range(LINKED) if face // BLOCK_FACES == index])
    for face in range(FACES):
        span = face_span(face)
        change = weights[2][0] * near[FACES + face] + weights[2][1] * local[:, span]
        keep_face_parts(more_parts, span, change)
        residual[:, span] = local[:, span] - penalty_weight * change
        traces[:, span] = traces[:, span] + direction[:, span] + near[FACES + face] + change
    for index in range(blocks):
        span = block_span(index)
        residual[:, span] = residual[:, span] - applied(index, more_parts, blocks)
    for index in range(linked_blocks, blocks):
        span = block_span(index)
        traces_out[span] = traces[:, span].T

    wait_arrived(2)
    for face in range(LINKED):
        span = face_span(face)
        view = landed_half[0, face].astype(jnp.float32) + penalty_weight * direction[:, span]
        beyond = there(face) * (weights[1][0] * near[face] + weights[1][1] * view)
        near[face] = beyond
        change = (weights[2][1] * penalty_weight) * beyond
        local[:, span] = change
        keep_face_parts(parts, span, change)

    for index in range(blocks):
        span = block_span(index)
        value = residual[:, span] - applied(index, parts, linked_blocks)
        if index < linked_blocks:
            for face in range(index * BLOCK_FACES, (index + 1) * BLOCK_FACES):
                lane = (face % BLOCK_FACES) * mode
                change = local[:, face_span(face)]
                mine = value[:, lane : lane + mode] + penalty_weight * (near[face] - change)
                residual_out[face_span(face)] = mine.T
                traces_out[face_span(face)] = (traces[:, face_span(face)] + change).T
        else:
            residual_out[span] = value.T
    for face in range(LINKED):
        span = face_span(face)
        view = landed_half[0, face].astype(jnp.float32) + penalty_weight * direction[:, span]
        landed[1, face] = view - guess_slope * near[face] + penalty_weight * near[FACES + face]

    wait_sent()
    wait_arrived(3)
    for face in range(LINKED):
        span = face_span(face)
        view = landed[1, face] + landed_half[1, face].astype(jnp.float32)
        beyond = weights[2][0] * near[face] + weights[2][1] * view
        beyond = (penalty_weight * there(face)) * beyond
        residual_out[span] = residual_out[span] + beyond.T


def write_kernel(traces, residual, traces_out, residual_out, sems):
    copies = [
        pltpu.make_async_copy(traces, traces_out, sems.at[0]),
        pltpu.make_async_copy(residual, residual_out, sems.at[1]),
    ]
    for copy in copies:
        copy.start()
    for copy in copies:
        copy.wait()


def in_hbm(value):
    return pltpu.with_memory_space_constraint(value, pltpu.HBM)


def on_device(
    axis_sizes, coupling, interior_inverse, boundary_stiffness, block_counts, initial_traces, trace_loads
):
    slots, trace_width, inner_width = coupling.shape[2:]
    load_width = initial_traces.shape[-1]
    mode = trace_width // FACES
    whole = pl.BlockSpec(memory_space=pltpu.HBM)
    vmem = pl.BlockSpec(memory_space=pltpu.VMEM)
    out = pltpu.VMEM((trace_width, load_width), jnp.float32)
    flat = pltpu.VMEM((load_width, trace_width), jnp.float32)
    square = pltpu.VMEM((trace_width, trace_width), jnp.bfloat16)
    long = pltpu.VMEM((trace_width, slots * inner_width), jnp.bfloat16)
    traces, residual = pl.pallas_call(
        functools.partial(kernel, axis_sizes),
        out_shape=(out, out),
        in_specs=[whole, whole, whole, pl.BlockSpec(memory_space=pltpu.SMEM), whole, whole],
        out_specs=(vmem, vmem),
        scratch_shapes=[
            long,
            pltpu.VMEM((slots, inner_width, inner_width), jnp.bfloat16),
            square,
            long,
            square,
            square,
            pltpu.VMEM((2, trace_width, load_width), jnp.float32),
            pltpu.VMEM((2 * load_width, trace_width), jnp.bfloat16),
            pltpu.VMEM((2 * load_width, trace_width), jnp.bfloat16),
            flat,
            flat,
            flat,
            flat,
            flat,
            pltpu.VMEM((2 * FACES, load_width, mode), jnp.float32),
            pltpu.VMEM((LINKED, load_width, mode), jnp.float32),
            pltpu.VMEM((2, LINKED, load_width, mode), jnp.bfloat16),
            pltpu.VMEM((2, LINKED, load_width, mode), jnp.float32),
            pltpu.VMEM((2, LINKED, load_width, mode), jnp.bfloat16),
            pltpu.VMEM((BLOCK_FACES * mode, trace_width), jnp.float32),
            pltpu.SemaphoreType.DMA((slots + 2 + inner_width * FACES // (BLOCK_FACES * trace_width),)),
            pltpu.SemaphoreType.DMA((1,)),
            pltpu.SemaphoreType.DMA((SWEEPS + 1,)),
        ],
        compiler_params=pltpu.CompilerParams(
            collective_id=0, has_side_effects=True, vmem_limit_bytes=48 << 20
        ),
        name="condense_and_sweep",
    )(
        in_hbm(coupling[0, 0]),
        in_hbm(interior_inverse[0, 0]),
        in_hbm(boundary_stiffness[0, 0]),
        block_counts,
        in_hbm(initial_traces[0, 0]),
        in_hbm(trace_loads[0, 0]),
    )
    result = jax.ShapeDtypeStruct((trace_width, load_width), jnp.float32)
    traces, residual = pl.pallas_call(
        write_kernel,
        out_shape=(result, result),
        in_specs=[vmem, vmem],
        out_specs=(whole, whole),
        scratch_shapes=[pltpu.SemaphoreType.DMA((2,))],
        name="write_results",
    )(
        pltpu.with_memory_space_constraint(traces, pltpu.VMEM),
        pltpu.with_memory_space_constraint(residual, pltpu.VMEM),
    )
    return (traces[None, None], residual[None, None])


def solution(mesh):
    in_specs = (
        P("gx", ("gy", "ha"), None, None, None),
        P("gx", ("gy", "ha"), None, None, None),
        P("gx", ("gy", "ha"), None, None),
        P("gx", ("gy", "ha")),
        P("gx", ("gy", "ha"), None, None),
        P("gx", ("gy", "ha"), None, None),
    )
    out_specs = (P("gx", ("gy", "ha"), None, None), P("gx", ("gy", "ha"), None, None))
    axis_sizes = (mesh.shape["gx"], mesh.shape["gy"], mesh.shape["ha"])
    return jax.shard_map(
        functools.partial(on_device, axis_sizes),
        mesh=mesh, in_specs=in_specs, out_specs=out_specs, check_vma=False,
    )
```

```python
import functools

import jax
import jax.numpy as jnp
from jax import lax
from jax.experimental import pallas as pl
from jax.experimental.pallas import tpu as pltpu
from jax.sharding import PartitionSpec as P

SWEEPS = 3
FACES = 6
LINKED = 4
BLOCK_FACES = 2
EARLY = 2
MEET = 0
NW = 256

penalty_weight = 2.0
lower_bound = 1.0
upper_bound = 14.0
spectrum_centre = (upper_bound + lower_bound) / 2.0
spectrum_half = (upper_bound - lower_bound) / 2.0
sigma_ratio = spectrum_centre / spectrum_half

guess_slope = 8.0


def sweep_weights():
    weights = [(0.0, 1.0 / spectrum_centre)]
    weight_old = 1.0 / sigma_ratio
    for _ in range(SWEEPS - 1):
        weight_new = 1.0 / (2.0 * sigma_ratio - weight_old)
        weights.append((weight_new * weight_old, 2.0 * weight_new / spectrum_half))
        weight_old = weight_new
    return weights


def two_parts(value):
    high = value.astype(jnp.bfloat16)
    low = (value - high.astype(jnp.float32)).astype(jnp.bfloat16)
    return high, low


def dot_nn(left, right):
    return lax.dot_general(left, right, (((1,), (0,)), ((), ())), preferred_element_type=jnp.float32)


def dot_nt(left, right):
    return lax.dot_general(left, right, (((1,), (1,)), ((), ())), preferred_element_type=jnp.float32)


def kernel(
    axis_sizes,
    coupling,
    inverse,
    stiffness,
    counts,
    initial,
    loads,
    traces_out,
    residual_out,
    wide,
    inv,
    stiff,
    products,
    a_high,
    a_low,
    given,
    parts,
    more_parts,
    traces,
    bound_t,
    residual,
    direction,
    local,
    near,
    sent,
    sent_half,
    landed,
    landed_half,
    total,
    in_sems,
    send_sems,
    recv_sems,
):
    slots, trace_width, inner_width = coupling.shape
    load_width = initial.shape[1]
    mode = trace_width // FACES
    block = BLOCK_FACES * mode
    blocks = trace_width // block
    rows, groups, halves = axis_sizes
    columns = groups * halves
    row = lax.axis_index("gx")
    column = lax.axis_index("gy") * halves + lax.axis_index("ha")

    def column_id(index):
        return {"gy": lax.div(index, halves), "ha": lax.rem(index, halves)}

    routes = (
        (0, 1, row > 0, {"gx": row - 1}),
        (1, 0, row + 1 < rows, {"gx": row + 1}),
        (2, 3, column > 0, column_id(column - 1)),
        (3, 2, column + 1 < columns, column_id(column + 1)),
    )

    def inner_span(slot):
        return pl.ds(slot * inner_width, inner_width)

    def coupling_copy(slot, start, size, sem):
        rows_of = pl.ds(start, size)
        pltpu.make_async_copy(coupling.at[slot, rows_of], wide.at[rows_of, inner_span(slot)], sem).start()

    def wait_for(place, sem):
        pltpu.make_async_copy(place, place, sem).wait()

    def block_span(index):
        return pl.ds(index * block, block)

    chunks = inner_width // block
    given_sem = in_sems.at[0]
    chunk_sems = [in_sems.at[1 + chunk] for chunk in range(chunks)]
    rest_sem, stiff_sem = in_sems.at[1 + chunks], in_sems.at[2 + chunks]
    slot_sems = [None] + [in_sems.at[2 + chunks + slot] for slot in range(1, slots)]
    coupling_copy(0, 0, block, chunk_sems[0])
    for chunk in range(chunks):
        piece = inv.at[0, pl.ds(chunk * block, block)]
        pltpu.make_async_copy(inverse.at[0, pl.ds(chunk * block, block)], piece, chunk_sems[chunk]).start()
    coupling_copy(0, block, trace_width - block, rest_sem)
    pltpu.make_async_copy(initial, given.at[0], given_sem).start()
    pltpu.make_async_copy(loads, given.at[1], given_sem).start()
    def load_slot(slot):
        coupling_copy(slot, 0, trace_width, slot_sems[slot])
        pltpu.make_async_copy(inverse.at[slot], inv.at[slot], slot_sems[slot]).start()

    def load_stiff():
        for index in range(blocks):
            part = (block_span(index), pl.ds(index * block, trace_width - index * block))
            pltpu.make_async_copy(stiffness.at[part], stiff.at[part], stiff_sem).start()

    load_slot(1)

    def wait_slot(slot):
        wait_for(inv.at[pl.ds(0, 2)], slot_sems[slot])

    barrier = pltpu.get_barrier_semaphore()
    partners = 0
    for _, _, exists, target in routes:
        partners = partners + exists.astype(jnp.int32)

        @pl.when(exists)
        def _():
            pl.semaphore_signal(barrier, inc=1, device_id=target, device_id_type=pl.DeviceIdType.MESH)

    for face, _, exists, _ in routes:

        @pl.when(jnp.logical_not(exists))
        def _():
            landed[:, face] = jnp.zeros((2, mode, load_width), jnp.float32)
            landed_half[:, face] = jnp.zeros((2, mode, load_width), jnp.bfloat16)

    def message(step, route):
        face, spot, _, target = route
        source = (
            initial.at[pl.ds(face * mode, mode)],
            sent.at[face],
            sent_half.at[0, face],
            sent_half.at[1, face],
        )[step]
        place = landed.at[step, spot] if step < 2 else landed_half.at[step - 2, spot]
        return pltpu.make_async_remote_copy(
            src_ref=source,
            dst_ref=place,
            send_sem=send_sems.at[0],
            recv_sem=recv_sems.at[step],
            device_id=target,
            device_id_type=pl.DeviceIdType.MESH,
        )

    def send(step, faces):
        for route in routes:
            if route[0] in faces:

                @pl.when(route[2])
                def _():
                    message(step, route).start()

    def wait_bytes(place, per_face, sem):
        for number in range(1, LINKED + 1):

            @pl.when(partners == number)
            def _():
                part = place.at[pl.ds(0, number * per_face)]
                pltpu.make_async_copy(part, part, sem).wait()

    def wait_arrived(step):
        place = landed.at[step] if step < 2 else landed_half.at[step - 2]
        wait_bytes(place, 1, recv_sems.at[step])

    def wait_sent():
        wait_bytes(near, 3, send_sems.at[0])

    def there(face):
        return jnp.where(routes[face][2], 1.0, 0.0)

    def face_span(face):
        return pl.ds(face * mode, mode)

    def block_rows(index):
        return slice(index * block, (index + 1) * block)

    weights = sweep_weights()

    def product_of(index, slot):
        span = block_span(index)
        if index == 0 and slot == 0:
            value = 0.0
            for chunk in range(chunks):
                wait_for(inv.at[0, pl.ds(0, block * (2 if chunk == 0 else 1))], chunk_sems[chunk])
                if chunk == 0:
                    load_slot(2)
                inside = pl.ds(chunk * block, block)
                value = value + dot_nn(wide[span, inside], inv[slot, inside])
        else:
            live = jnp.where(counts[0, 0] > slot, 1.0, 0.0)
            for piece in range(inner_width // NW):
                inside = pl.ds(piece * NW, NW)
                value = dot_nn(wide[span, inner_span(slot)], inv[slot, :, inside]) * live
                products[span, pl.ds(slot * inner_width + piece * NW, NW)] = value.astype(jnp.bfloat16)
            return
        value = value * jnp.where(counts[0, 0] > slot, 1.0, 0.0)
        products[span, inner_span(slot)] = value.astype(jnp.bfloat16)

    def keep_condensed(index, other, value):
        span, place = block_span(index), block_span(other)
        value = stiff[span, place].astype(jnp.float32) - value
        a_high[span, place], a_low[span, place] = two_parts(value)

    def condense_first(slot):
        for other in range(blocks):
            place = block_span(other)
            value = dot_nt(products[block_span(0), inner_span(slot)], wide[place, inner_span(slot)])
            if slot > 0:
                value = value + total[:, place]
            if slot + 1 < slots:
                total[:, place] = value
            else:
                keep_condensed(0, other, value)

    def condense(index):
        for other in range(index, blocks):
            keep_condensed(index, other, dot_nt(products[block_span(index), :], wide[block_span(other), :]))

    def applied(index, source, depth):
        span = block_span(index)
        ones = pl.ds(0, load_width)
        both, rest = [], []
        if index < depth:
            after = pl.ds(index * block, (depth - index) * block)
            both.append(dot_nt(source[:, after], a_high[span, after]))
            rest.append(dot_nt(source[ones, after], a_low[span, after]))
        if index > 0:
            before = pl.ds(0, min(index, depth) * block)
            both.append(dot_nn(source[:, before], a_high[before, span]))
            rest.append(dot_nn(source[ones, before], a_low[before, span]))
        both, rest = sum(both[1:], both[0]), sum(rest[1:], rest[0])
        return both[:load_width] + both[load_width:] + rest

    def keep_face_parts(place, span, value):
        high, low = two_parts(value)
        place[pl.ds(0, load_width), span] = high
        place[pl.ds(load_width, load_width), span] = low

    def keep_parts(value):
        high, low = two_parts(value)
        parts[pl.ds(0, load_width)] = high
        parts[pl.ds(load_width, load_width)] = low

    for slot in range(slots):
        if slot > 0:
            wait_slot(slot)
        product_of(0, slot)
        if slot == MEET:
            pl.semaphore_wait(barrier, partners)
            send(0, range(LINKED))
        if slot == 0:
            wait_for(wide.at[pl.ds(0, trace_width - block), inner_span(0)], rest_sem)
            load_slot(3)
            load_stiff()
        if slot < EARLY:
            product_of(1, slot)
        if slot == 0:
            wait_for(given, given_sem)
            start = given[0].T
            traces[...] = start
            keep_parts(start)
            bound_t[...] = given[1].T
        if slot + 1 == slots:
            wait_for(stiff.at[pl.ds(0, (trace_width + block) // 2)], stiff_sem)
        condense_first(slot)

    linked_blocks = LINKED // BLOCK_FACES
    for index in range(blocks):
        if index > 0:
            for slot in range(EARLY if index == 1 else 0, slots):
                product_of(index, slot)
            condense(index)
        span = block_span(index)
        value = bound_t[:, span] - applied(index, parts, blocks) - penalty_weight * traces[:, span]
        if index < linked_blocks:
            local[:, span] = value
            faces = range(index * BLOCK_FACES, (index + 1) * BLOCK_FACES)
            for face in faces:
                sent[face] = value[:, (face % BLOCK_FACES) * mode : (face % BLOCK_FACES + 1) * mode]
            send(1, faces)
        else:
            residual[:, span] = value
            change = weights[0][1] * value
            direction[:, span] = change
            keep_face_parts(more_parts, span, change)
        if index + 1 == linked_blocks:
            wait_arrived(0)
            for face in range(LINKED):
                span = face_span(face)
                value = local[:, span] + penalty_weight * landed[0, face].T
                residual[:, span] = value
                change = weights[0][1] * value
                direction[:, span] = change
                keep_face_parts(more_parts, span, change)

    for index in range(blocks):
        span = block_span(index)
        value = residual[:, span] - applied(index, more_parts, blocks) - penalty_weight * direction[:, span]
        local[:, span] = value
        faces = [face for face in range(LINKED) if face // BLOCK_FACES == index]
        for face in faces:
            sent_half[0, face] = value[
                :, (face % BLOCK_FACES) * mode : (face % BLOCK_FACES + 1) * mode
            ].astype(jnp.bfloat16)
        send(2, faces)

    wait_arrived(1)
    for face in range(FACES):
        span = face_span(face)
        value = local[:, span]
        if face < LINKED:
            beyond = (weights[0][1] * there(face)) * (landed[1, face] + penalty_weight * traces[:, span])
            near[face] = beyond
            value = value + penalty_weight * beyond
        change = weights[1][0] * direction[:, span] + weights[1][1] * value
        residual[:, span] = value
        near[FACES + face] = change
        keep_face_parts(parts, span, change)

    for index in range(blocks):
        value = applied(index, parts, blocks)
        for face in range(index * BLOCK_FACES, (index + 1) * BLOCK_FACES):
            span = face_span(face)
            lane = (face % BLOCK_FACES) * mode
            mine = residual[:, span] - value[:, lane : lane + mode] - penalty_weight * near[FACES + face]
            local[:, span] = mine
            if face < LINKED:
                view = sent_half[0, face].astype(jnp.float32) + penalty_weight * near[face]
                view_change = weights[1][0] * direction[:, span] + weights[1][1] * view
                sent_half[1, face] = (mine - (view - guess_slope * view_change)).astype(jnp.bfloat16)
        send(3, [face for face in range(LINKED) if face // BLOCK_FACES == index])
    for face in range(FACES):
        span = face_span(face)
        change = weights[2][0] * near[FACES + face] + weights[2][1] * local[:, span]
        keep_face_parts(more_parts, span, change)
        residual[:, span] = local[:, span] - penalty_weight * change
        traces[:, span] = traces[:, span] + direction[:, span] + near[FACES + face] + change
    for index in range(blocks):
        span = block_span(index)
        residual[:, span] = residual[:, span] - applied(index, more_parts, blocks)
    for index in range(linked_blocks, blocks):
        span = block_span(index)
        traces_out[span] = traces[:, span].T

    wait_arrived(2)
    for face in range(LINKED):
        span = face_span(face)
        view = landed_half[0, face].astype(jnp.float32) + penalty_weight * direction[:, span]
        beyond = there(face) * (weights[1][0] * near[face] + weights[1][1] * view)
        near[face] = beyond
        change = (weights[2][1] * penalty_weight) * beyond
        local[:, span] = change
        keep_face_parts(parts, span, change)

    for index in range(blocks):
        span = block_span(index)
        value = residual[:, span] - applied(index, parts, linked_blocks)
        if index < linked_blocks:
            for face in range(index * BLOCK_FACES, (index + 1) * BLOCK_FACES):
                lane = (face % BLOCK_FACES) * mode
                change = local[:, face_span(face)]
                mine = value[:, lane : lane + mode] + penalty_weight * (near[face] - change)
                residual_out[face_span(face)] = mine.T
                traces_out[face_span(face)] = (traces[:, face_span(face)] + change).T
        else:
            residual_out[span] = value.T
    for face in range(LINKED):
        span = face_span(face)
        view = landed_half[0, face].astype(jnp.float32) + penalty_weight * direction[:, span]
        landed[1, face] = view - guess_slope * near[face] + penalty_weight * near[FACES + face]

    wait_sent()
    wait_arrived(3)
    for face in range(LINKED):
        span = face_span(face)
        view = landed[1, face] + landed_half[1, face].astype(jnp.float32)
        beyond = weights[2][0] * near[face] + weights[2][1] * view
        beyond = (penalty_weight * there(face)) * beyond
        residual_out[span] = residual_out[span] + beyond.T


def write_kernel(traces, residual, traces_out, residual_out, sems):
    copies = [
        pltpu.make_async_copy(traces, traces_out, sems.at[0]),
        pltpu.make_async_copy(residual, residual_out, sems.at[1]),
    ]
    for copy in copies:
        copy.start()
    for copy in copies:
        copy.wait()


def in_hbm(value):
    return pltpu.with_memory_space_constraint(value, pltpu.HBM)


def on_device(
    axis_sizes, coupling, interior_inverse, boundary_stiffness, block_counts, initial_traces, trace_loads
):
    slots, trace_width, inner_width = coupling.shape[2:]
    load_width = initial_traces.shape[-1]
    mode = trace_width // FACES
    whole = pl.BlockSpec(memory_space=pltpu.HBM)
    vmem = pl.BlockSpec(memory_space=pltpu.VMEM)
    out = pltpu.VMEM((trace_width, load_width), jnp.float32)
    flat = pltpu.VMEM((load_width, trace_width), jnp.float32)
    square = pltpu.VMEM((trace_width, trace_width), jnp.bfloat16)
    long = pltpu.VMEM((trace_width, slots * inner_width), jnp.bfloat16)
    traces, residual = pl.pallas_call(
        functools.partial(kernel, axis_sizes),
        out_shape=(out, out),
        in_specs=[whole, whole, whole, pl.BlockSpec(memory_space=pltpu.SMEM), whole, whole],
        out_specs=(vmem, vmem),
        scratch_shapes=[
            long,
            pltpu.VMEM((slots, inner_width, inner_width), jnp.bfloat16),
            square,
            long,
            square,
            square,
            pltpu.VMEM((2, trace_width, load_width), jnp.float32),
            pltpu.VMEM((2 * load_width, trace_width), jnp.bfloat16),
            pltpu.VMEM((2 * load_width, trace_width), jnp.bfloat16),
            flat,
            flat,
            flat,
            flat,
            flat,
            pltpu.VMEM((2 * FACES, load_width, mode), jnp.float32),
            pltpu.VMEM((LINKED, load_width, mode), jnp.float32),
            pltpu.VMEM((2, LINKED, load_width, mode), jnp.bfloat16),
            pltpu.VMEM((2, LINKED, load_width, mode), jnp.float32),
            pltpu.VMEM((2, LINKED, load_width, mode), jnp.bfloat16),
            pltpu.VMEM((BLOCK_FACES * mode, trace_width), jnp.float32),
            pltpu.SemaphoreType.DMA((slots + 2 + inner_width * FACES // (BLOCK_FACES * trace_width),)),
            pltpu.SemaphoreType.DMA((1,)),
            pltpu.SemaphoreType.DMA((SWEEPS + 1,)),
        ],
        compiler_params=pltpu.CompilerParams(
            collective_id=0, has_side_effects=True, vmem_limit_bytes=48 << 20
        ),
        name="condense_and_sweep",
    )(
        in_hbm(coupling[0, 0]),
        in_hbm(interior_inverse[0, 0]),
        in_hbm(boundary_stiffness[0, 0]),
        block_counts,
        in_hbm(initial_traces[0, 0]),
        in_hbm(trace_loads[0, 0]),
    )
    result = jax.ShapeDtypeStruct((trace_width, load_width), jnp.float32)
    traces, residual = pl.pallas_call(
        write_kernel,
        out_shape=(result, result),
        in_specs=[vmem, vmem],
        out_specs=(whole, whole),
        scratch_shapes=[pltpu.SemaphoreType.DMA((2,))],
        name="write_results",
    )(
        pltpu.with_memory_space_constraint(traces, pltpu.VMEM),
        pltpu.with_memory_space_constraint(residual, pltpu.VMEM),
    )
    return (traces[None, None], residual[None, None])


def solution(mesh):
    in_specs = (
        P("gx", ("gy", "ha"), None, None, None),
        P("gx", ("gy", "ha"), None, None, None),
        P("gx", ("gy", "ha"), None, None),
        P("gx", ("gy", "ha")),
        P("gx", ("gy", "ha"), None, None),
        P("gx", ("gy", "ha"), None, None),
    )
    out_specs = (P("gx", ("gy", "ha"), None, None), P("gx", ("gy", "ha"), None, None))
    axis_sizes = (mesh.shape["gx"], mesh.shape["gy"], mesh.shape["ha"])
    return jax.shard_map(
        functools.partial(on_device, axis_sizes),
        mesh=mesh, in_specs=in_specs, out_specs=out_specs, check_vma=False,
    )
```

```python
import functools

import jax
import jax.numpy as jnp
from jax import lax
from jax.experimental import pallas as pl
from jax.experimental.pallas import tpu as pltpu
from jax.sharding import PartitionSpec as P

SWEEPS = 3
FACES = 6
LINKED = 4
BLOCK_FACES = 2
EARLY = 3
MEET = 0
NW = 256

penalty_weight = 2.0
lower_bound = 1.0
upper_bound = 14.0
spectrum_centre = (upper_bound + lower_bound) / 2.0
spectrum_half = (upper_bound - lower_bound) / 2.0
sigma_ratio = spectrum_centre / spectrum_half

guess_slope = 8.0


def sweep_weights():
    weights = [(0.0, 1.0 / spectrum_centre)]
    weight_old = 1.0 / sigma_ratio
    for _ in range(SWEEPS - 1):
        weight_new = 1.0 / (2.0 * sigma_ratio - weight_old)
        weights.append((weight_new * weight_old, 2.0 * weight_new / spectrum_half))
        weight_old = weight_new
    return weights


def two_parts(value):
    high = value.astype(jnp.bfloat16)
    low = (value - high.astype(jnp.float32)).astype(jnp.bfloat16)
    return high, low


def dot_nn(left, right):
    return lax.dot_general(left, right, (((1,), (0,)), ((), ())), preferred_element_type=jnp.float32)


def dot_nt(left, right):
    return lax.dot_general(left, right, (((1,), (1,)), ((), ())), preferred_element_type=jnp.float32)


def kernel(
    axis_sizes,
    coupling,
    inverse,
    stiffness,
    counts,
    initial,
    loads,
    traces_out,
    residual_out,
    wide,
    inv,
    stiff,
    products,
    a_high,
    a_low,
    given,
    parts,
    more_parts,
    traces,
    bound_t,
    residual,
    direction,
    local,
    near,
    sent,
    sent_half,
    landed,
    landed_half,
    total,
    in_sems,
    send_sems,
    recv_sems,
):
    slots, trace_width, inner_width = coupling.shape
    load_width = initial.shape[1]
    mode = trace_width // FACES
    block = BLOCK_FACES * mode
    blocks = trace_width // block
    rows, groups, halves = axis_sizes
    columns = groups * halves
    row = lax.axis_index("gx")
    column = lax.axis_index("gy") * halves + lax.axis_index("ha")

    def column_id(index):
        return {"gy": lax.div(index, halves), "ha": lax.rem(index, halves)}

    routes = (
        (0, 1, row > 0, {"gx": row - 1}),
        (1, 0, row + 1 < rows, {"gx": row + 1}),
        (2, 3, column > 0, column_id(column - 1)),
        (3, 2, column + 1 < columns, column_id(column + 1)),
    )

    def inner_span(slot):
        return pl.ds(slot * inner_width, inner_width)

    def coupling_copy(slot, start, size, sem):
        rows_of = pl.ds(start, size)
        pltpu.make_async_copy(coupling.at[slot, rows_of], wide.at[rows_of, inner_span(slot)], sem).start()

    def wait_for(place, sem):
        pltpu.make_async_copy(place, place, sem).wait()

    def block_span(index):
        return pl.ds(index * block, block)

    chunks = inner_width // block
    given_sem = in_sems.at[0]
    chunk_sems = [in_sems.at[1 + chunk] for chunk in range(chunks)]
    rest_sem, stiff_sem = in_sems.at[1 + chunks], in_sems.at[2 + chunks]
    slot_sems = [None] + [in_sems.at[2 + chunks + slot] for slot in range(1, slots)]
    coupling_copy(0, 0, block, chunk_sems[0])
    for chunk in range(chunks):
        piece = inv.at[0, pl.ds(chunk * block, block)]
        pltpu.make_async_copy(inverse.at[0, pl.ds(chunk * block, block)], piece, chunk_sems[chunk]).start()
    coupling_copy(0, block, trace_width - block, rest_sem)
    pltpu.make_async_copy(initial, given.at[0], given_sem).start()
    pltpu.make_async_copy(loads, given.at[1], given_sem).start()
    def load_slot(slot):
        coupling_copy(slot, 0, trace_width, slot_sems[slot])
        pltpu.make_async_copy(inverse.at[slot], inv.at[slot], slot_sems[slot]).start()

    def load_stiff():
        for index in range(blocks):
            part = (block_span(index), pl.ds(index * block, trace_width - index * block))
            pltpu.make_async_copy(stiffness.at[part], stiff.at[part], stiff_sem).start()

    load_slot(1)

    def wait_slot(slot):
        wait_for(inv.at[pl.ds(0, 2)], slot_sems[slot])

    barrier = pltpu.get_barrier_semaphore()
    partners = 0
    for _, _, exists, target in routes:
        partners = partners + exists.astype(jnp.int32)

        @pl.when(exists)
        def _():
            pl.semaphore_signal(barrier, inc=1, device_id=target, device_id_type=pl.DeviceIdType.MESH)

    for face, _, exists, _ in routes:

        @pl.when(jnp.logical_not(exists))
        def _():
            landed[:, face] = jnp.zeros((2, mode, load_width), jnp.float32)
            landed_half[:, face] = jnp.zeros((2, mode, load_width), jnp.bfloat16)

    def message(step, route):
        face, spot, _, target = route
        source = (
            initial.at[pl.ds(face * mode, mode)],
            sent.at[face],
            sent_half.at[0, face],
            sent_half.at[1, face],
        )[step]
        place = landed.at[step, spot] if step < 2 else landed_half.at[step - 2, spot]
        return pltpu.make_async_remote_copy(
            src_ref=source,
            dst_ref=place,
            send_sem=send_sems.at[0],
            recv_sem=recv_sems.at[step],
            device_id=target,
            device_id_type=pl.DeviceIdType.MESH,
        )

    def send(step, faces):
        for route in routes:
            if route[0] in faces:

                @pl.when(route[2])
                def _():
                    message(step, route).start()

    def wait_bytes(place, per_face, sem):
        for number in range(1, LINKED + 1):

            @pl.when(partners == number)
            def _():
                part = place.at[pl.ds(0, number * per_face)]
                pltpu.make_async_copy(part, part, sem).wait()

    def wait_arrived(step):
        place = landed.at[step] if step < 2 else landed_half.at[step - 2]
        wait_bytes(place, 1, recv_sems.at[step])

    def wait_sent():
        wait_bytes(near, 3, send_sems.at[0])

    def there(face):
        return jnp.where(routes[face][2], 1.0, 0.0)

    def face_span(face):
        return pl.ds(face * mode, mode)

    def block_rows(index):
        return slice(index * block, (index + 1) * block)

    weights = sweep_weights()

    def product_of(index, slot):
        span = block_span(index)
        if index == 0 and slot == 0:
            value = 0.0
            for chunk in range(chunks):
                wait_for(inv.at[0, pl.ds(0, block * (2 if chunk == 0 else 1))], chunk_sems[chunk])
                if chunk == 0:
                    load_slot(2)
                inside = pl.ds(chunk * block, block)
                value = value + dot_nn(wide[span, inside], inv[slot, inside])
        else:
            live = jnp.where(counts[0, 0] > slot, 1.0, 0.0)
            for piece in range(inner_width // NW):
                inside = pl.ds(piece * NW, NW)
                value = dot_nn(wide[span, inner_span(slot)], inv[slot, :, inside]) * live
                products[span, pl.ds(slot * inner_width + piece * NW, NW)] = value.astype(jnp.bfloat16)
            return
        value = value * jnp.where(counts[0, 0] > slot, 1.0, 0.0)
        products[span, inner_span(slot)] = value.astype(jnp.bfloat16)

    def keep_condensed(index, other, value):
        span, place = block_span(index), block_span(other)
        value = stiff[span, place].astype(jnp.float32) - value
        a_high[span, place], a_low[span, place] = two_parts(value)

    def condense_first(slot):
        for other in range(blocks):
            place = block_span(other)
            value = dot_nt(products[block_span(0), inner_span(slot)], wide[place, inner_span(slot)])
            if slot > 0:
                value = value + total[:, place]
            if slot + 1 < slots:
                total[:, place] = value
            else:
                keep_condensed(0, other, value)

    def condense(index):
        for other in range(index, blocks):
            keep_condensed(index, other, dot_nt(products[block_span(index), :], wide[block_span(other), :]))

    def applied(index, source, depth):
        span = block_span(index)
        ones = pl.ds(0, load_width)
        both, rest = [], []
        if index < depth:
            after = pl.ds(index * block, (depth - index) * block)
            both.append(dot_nt(source[:, after], a_high[span, after]))
            rest.append(dot_nt(source[ones, after], a_low[span, after]))
        if index > 0:
            before = pl.ds(0, min(index, depth) * block)
            both.append(dot_nn(source[:, before], a_high[before, span]))
            rest.append(dot_nn(source[ones, before], a_low[before, span]))
        both, rest = sum(both[1:], both[0]), sum(rest[1:], rest[0])
        return both[:load_width] + both[load_width:] + rest

    def keep_face_parts(place, span, value):
        high, low = two_parts(value)
        place[pl.ds(0, load_width), span] = high
        place[pl.ds(load_width, load_width), span] = low

    def keep_parts(value):
        high, low = two_parts(value)
        parts[pl.ds(0, load_width)] = high
        parts[pl.ds(load_width, load_width)] = low

    for slot in range(slots):
        if slot > 0:
            wait_slot(slot)
        if slot + 1 == slots:
            wait_for(stiff.at[pl.ds(0, (trace_width + block) // 2)], stiff_sem)
        product_of(0, slot)
        if slot == MEET:
            pl.semaphore_wait(barrier, partners)
            send(0, range(LINKED))
        if slot == 0:
            wait_for(wide.at[pl.ds(0, trace_width - block), inner_span(0)], rest_sem)
            wait_for(given, given_sem)
            load_slot(3)
            load_stiff()
        if slot < EARLY:
            product_of(1, slot)
        if slot == 0:
            start = given[0].T
            traces[...] = start
            keep_parts(start)
            bound_t[...] = given[1].T
        condense_first(slot)

    linked_blocks = LINKED // BLOCK_FACES
    for index in range(blocks):
        if index > 0:
            for slot in range(EARLY if index == 1 else 0, slots):
                product_of(index, slot)
            condense(index)
        span = block_span(index)
        value = bound_t[:, span] - applied(index, parts, blocks) - penalty_weight * traces[:, span]
        if index < linked_blocks:
            local[:, span] = value
            faces = range(index * BLOCK_FACES, (index + 1) * BLOCK_FACES)
            for face in faces:
                sent[face] = value[:, (face % BLOCK_FACES) * mode : (face % BLOCK_FACES + 1) * mode]
            send(1, faces)
        else:
            residual[:, span] = value
            change = weights[0][1] * value
            direction[:, span] = change
            keep_face_parts(more_parts, span, change)
        if index + 1 == linked_blocks:
            wait_arrived(0)
            for face in range(LINKED):
                span = face_span(face)
                value = local[:, span] + penalty_weight * landed[0, face].T
                residual[:, span] = value
                change = weights[0][1] * value
                direction[:, span] = change
                keep_face_parts(more_parts, span, change)

    for index in range(blocks):
        span = block_span(index)
        value = residual[:, span] - applied(index, more_parts, blocks) - penalty_weight * direction[:, span]
        local[:, span] = value
        faces = [face for face in range(LINKED) if face // BLOCK_FACES == index]
        for face in faces:
            sent_half[0, face] = value[
                :, (face % BLOCK_FACES) * mode : (face % BLOCK_FACES + 1) * mode
            ].astype(jnp.bfloat16)
        send(2, faces)

    wait_arrived(1)
    for face in range(FACES):
        span = face_span(face)
        value = local[:, span]
        if face < LINKED:
            beyond = (weights[0][1] * there(face)) * (landed[1, face] + penalty_weight * traces[:, span])
            near[face] = beyond
            value = value + penalty_weight * beyond
        change = weights[1][0] * direction[:, span] + weights[1][1] * value
        residual[:, span] = value
        near[FACES + face] = change
        keep_face_parts(parts, span, change)

    for index in range(blocks):
        value = applied(index, parts, blocks)
        for face in range(index * BLOCK_FACES, (index + 1) * BLOCK_FACES):
            span = face_span(face)
            lane = (face % BLOCK_FACES) * mode
            mine = residual[:, span] - value[:, lane : lane + mode] - penalty_weight * near[FACES + face]
            local[:, span] = mine
            if face < LINKED:
                view = sent_half[0, face].astype(jnp.float32) + penalty_weight * near[face]
                view_change = weights[1][0] * direction[:, span] + weights[1][1] * view
                sent_half[1, face] = (mine - (view - guess_slope * view_change)).astype(jnp.bfloat16)
        send(3, [face for face in range(LINKED) if face // BLOCK_FACES == index])
    for face in range(FACES):
        span = face_span(face)
        change = weights[2][0] * near[FACES + face] + weights[2][1] * local[:, span]
        keep_face_parts(more_parts, span, change)
        residual[:, span] = local[:, span] - penalty_weight * change
        traces[:, span] = traces[:, span] + direction[:, span] + near[FACES + face] + change
    for index in range(blocks):
        span = block_span(index)
        residual[:, span] = residual[:, span] - applied(index, more_parts, blocks)
    for index in range(linked_blocks, blocks):
        span = block_span(index)
        traces_out[span] = traces[:, span].T

    wait_arrived(2)
    for face in range(LINKED):
        span = face_span(face)
        view = landed_half[0, face].astype(jnp.float32) + penalty_weight * direction[:, span]
        beyond = there(face) * (weights[1][0] * near[face] + weights[1][1] * view)
        near[face] = beyond
        change = (weights[2][1] * penalty_weight) * beyond
        local[:, span] = change
        keep_face_parts(parts, span, change)

    for index in range(blocks):
        span = block_span(index)
        value = residual[:, span] - applied(index, parts, linked_blocks)
        if index < linked_blocks:
            for face in range(index * BLOCK_FACES, (index + 1) * BLOCK_FACES):
                lane = (face % BLOCK_FACES) * mode
                change = local[:, face_span(face)]
                mine = value[:, lane : lane + mode] + penalty_weight * (near[face] - change)
                residual_out[face_span(face)] = mine.T
                traces_out[face_span(face)] = (traces[:, face_span(face)] + change).T
        else:
            residual_out[span] = value.T
    for face in range(LINKED):
        span = face_span(face)
        view = landed_half[0, face].astype(jnp.float32) + penalty_weight * direction[:, span]
        landed[1, face] = view - guess_slope * near[face] + penalty_weight * near[FACES + face]

    wait_sent()
    wait_arrived(3)
    for face in range(LINKED):
        span = face_span(face)
        view = landed[1, face] + landed_half[1, face].astype(jnp.float32)
        beyond = weights[2][0] * near[face] + weights[2][1] * view
        beyond = (penalty_weight * there(face)) * beyond
        residual_out[span] = residual_out[span] + beyond.T


def write_kernel(traces, residual, traces_out, residual_out, sems):
    copies = [
        pltpu.make_async_copy(traces, traces_out, sems.at[0]),
        pltpu.make_async_copy(residual, residual_out, sems.at[1]),
    ]
    for copy in copies:
        copy.start()
    for copy in copies:
        copy.wait()


def in_hbm(value):
    return pltpu.with_memory_space_constraint(value, pltpu.HBM)


def on_device(
    axis_sizes, coupling, interior_inverse, boundary_stiffness, block_counts, initial_traces, trace_loads
):
    slots, trace_width, inner_width = coupling.shape[2:]
    load_width = initial_traces.shape[-1]
    mode = trace_width // FACES
    whole = pl.BlockSpec(memory_space=pltpu.HBM)
    vmem = pl.BlockSpec(memory_space=pltpu.VMEM)
    out = pltpu.VMEM((trace_width, load_width), jnp.float32)
    flat = pltpu.VMEM((load_width, trace_width), jnp.float32)
    square = pltpu.VMEM((trace_width, trace_width), jnp.bfloat16)
    long = pltpu.VMEM((trace_width, slots * inner_width), jnp.bfloat16)
    traces, residual = pl.pallas_call(
        functools.partial(kernel, axis_sizes),
        out_shape=(out, out),
        in_specs=[whole, whole, whole, pl.BlockSpec(memory_space=pltpu.SMEM), whole, whole],
        out_specs=(vmem, vmem),
        scratch_shapes=[
            long,
            pltpu.VMEM((slots, inner_width, inner_width), jnp.bfloat16),
            square,
            long,
            square,
            square,
            pltpu.VMEM((2, trace_width, load_width), jnp.float32),
            pltpu.VMEM((2 * load_width, trace_width), jnp.bfloat16),
            pltpu.VMEM((2 * load_width, trace_width), jnp.bfloat16),
            flat,
            flat,
            flat,
            flat,
            flat,
            pltpu.VMEM((2 * FACES, load_width, mode), jnp.float32),
            pltpu.VMEM((LINKED, load_width, mode), jnp.float32),
            pltpu.VMEM((2, LINKED, load_width, mode), jnp.bfloat16),
            pltpu.VMEM((2, LINKED, load_width, mode), jnp.float32),
            pltpu.VMEM((2, LINKED, load_width, mode), jnp.bfloat16),
            pltpu.VMEM((BLOCK_FACES * mode, trace_width), jnp.float32),
            pltpu.SemaphoreType.DMA((slots + 2 + inner_width * FACES // (BLOCK_FACES * trace_width),)),
            pltpu.SemaphoreType.DMA((1,)),
            pltpu.SemaphoreType.DMA((SWEEPS + 1,)),
        ],
        compiler_params=pltpu.CompilerParams(
            collective_id=0, has_side_effects=True, vmem_limit_bytes=48 << 20
        ),
        name="condense_and_sweep",
    )(
        in_hbm(coupling[0, 0]),
        in_hbm(interior_inverse[0, 0]),
        in_hbm(boundary_stiffness[0, 0]),
        block_counts,
        in_hbm(initial_traces[0, 0]),
        in_hbm(trace_loads[0, 0]),
    )
    result = jax.ShapeDtypeStruct((trace_width, load_width), jnp.float32)
    traces, residual = pl.pallas_call(
        write_kernel,
        out_shape=(result, result),
        in_specs=[vmem, vmem],
        out_specs=(whole, whole),
        scratch_shapes=[pltpu.SemaphoreType.DMA((2,))],
        name="write_results",
    )(
        pltpu.with_memory_space_constraint(traces, pltpu.VMEM),
        pltpu.with_memory_space_constraint(residual, pltpu.VMEM),
    )
    return (traces[None, None], residual[None, None])


def solution(mesh):
    in_specs = (
        P("gx", ("gy", "ha"), None, None, None),
        P("gx", ("gy", "ha"), None, None, None),
        P("gx", ("gy", "ha"), None, None),
        P("gx", ("gy", "ha")),
        P("gx", ("gy", "ha"), None, None),
        P("gx", ("gy", "ha"), None, None),
    )
    out_specs = (P("gx", ("gy", "ha"), None, None), P("gx", ("gy", "ha"), None, None))
    axis_sizes = (mesh.shape["gx"], mesh.shape["gy"], mesh.shape["ha"])
    return jax.shard_map(
        functools.partial(on_device, axis_sizes),
        mesh=mesh, in_specs=in_specs, out_specs=out_specs, check_vma=False,
    )
```

```python
import functools

import jax
import jax.numpy as jnp
from jax import lax
from jax.experimental import pallas as pl
from jax.experimental.pallas import tpu as pltpu
from jax.sharding import PartitionSpec as P

SWEEPS = 3
FACES = 6
LINKED = 4
BLOCK_FACES = 2
EARLY = 3
MEET = 0
NW = 256

penalty_weight = 2.0
lower_bound = 1.0
upper_bound = 14.0
spectrum_centre = (upper_bound + lower_bound) / 2.0
spectrum_half = (upper_bound - lower_bound) / 2.0
sigma_ratio = spectrum_centre / spectrum_half

guess_slope = 8.0


def sweep_weights():
    weights = [(0.0, 1.0 / spectrum_centre)]
    weight_old = 1.0 / sigma_ratio
    for _ in range(SWEEPS - 1):
        weight_new = 1.0 / (2.0 * sigma_ratio - weight_old)
        weights.append((weight_new * weight_old, 2.0 * weight_new / spectrum_half))
        weight_old = weight_new
    return weights


def two_parts(value):
    high = value.astype(jnp.bfloat16)
    low = (value - high.astype(jnp.float32)).astype(jnp.bfloat16)
    return high, low


def dot_nn(left, right):
    return lax.dot_general(left, right, (((1,), (0,)), ((), ())), preferred_element_type=jnp.float32)


def dot_nt(left, right):
    return lax.dot_general(left, right, (((1,), (1,)), ((), ())), preferred_element_type=jnp.float32)


def kernel(
    axis_sizes,
    coupling,
    inverse,
    stiffness,
    counts,
    initial,
    loads,
    traces_out,
    residual_out,
    wide,
    inv,
    stiff,
    products,
    a_high,
    a_low,
    given,
    parts,
    more_parts,
    traces,
    bound_t,
    residual,
    direction,
    local,
    near,
    sent,
    sent_half,
    landed,
    landed_half,
    total,
    in_sems,
    send_sems,
    recv_sems,
):
    slots, trace_width, inner_width = coupling.shape
    load_width = initial.shape[1]
    mode = trace_width // FACES
    block = BLOCK_FACES * mode
    blocks = trace_width // block
    rows, groups, halves = axis_sizes
    columns = groups * halves
    row = lax.axis_index("gx")
    column = lax.axis_index("gy") * halves + lax.axis_index("ha")

    def column_id(index):
        return {"gy": lax.div(index, halves), "ha": lax.rem(index, halves)}

    routes = (
        (0, 1, row > 0, {"gx": row - 1}),
        (1, 0, row + 1 < rows, {"gx": row + 1}),
        (2, 3, column > 0, column_id(column - 1)),
        (3, 2, column + 1 < columns, column_id(column + 1)),
    )

    def inner_span(slot):
        return pl.ds(slot * inner_width, inner_width)

    def coupling_copy(slot, start, size, sem):
        rows_of = pl.ds(start, size)
        pltpu.make_async_copy(coupling.at[slot, rows_of], wide.at[rows_of, inner_span(slot)], sem).start()

    def wait_for(place, sem):
        pltpu.make_async_copy(place, place, sem).wait()

    def block_span(index):
        return pl.ds(index * block, block)

    chunks = inner_width // block
    given_sem = in_sems.at[0]
    chunk_sems = [in_sems.at[1 + chunk] for chunk in range(chunks)]
    rest_sem, stiff_sem = in_sems.at[1 + chunks], in_sems.at[2 + chunks]
    slot_sems = [None] + [in_sems.at[2 + chunks + slot] for slot in range(1, slots)]
    coupling_copy(0, 0, block, chunk_sems[0])
    for chunk in range(chunks):
        piece = inv.at[0, pl.ds(chunk * block, block)]
        pltpu.make_async_copy(inverse.at[0, pl.ds(chunk * block, block)], piece, chunk_sems[chunk]).start()
    coupling_copy(0, block, trace_width - block, rest_sem)
    pltpu.make_async_copy(initial, given.at[0], given_sem).start()
    pltpu.make_async_copy(loads, given.at[1], given_sem).start()
    def load_slot(slot):
        coupling_copy(slot, 0, trace_width, slot_sems[slot])
        pltpu.make_async_copy(inverse.at[slot], inv.at[slot], slot_sems[slot]).start()

    def load_stiff():
        for index in range(blocks):
            part = (block_span(index), pl.ds(index * block, trace_width - index * block))
            pltpu.make_async_copy(stiffness.at[part], stiff.at[part], stiff_sem).start()

    load_slot(1)

    def wait_slot(slot):
        wait_for(inv.at[pl.ds(0, 2)], slot_sems[slot])

    barrier = pltpu.get_barrier_semaphore()
    partners = 0
    for _, _, exists, target in routes:
        partners = partners + exists.astype(jnp.int32)

        @pl.when(exists)
        def _():
            pl.semaphore_signal(barrier, inc=1, device_id=target, device_id_type=pl.DeviceIdType.MESH)

    for face, _, exists, _ in routes:

        @pl.when(jnp.logical_not(exists))
        def _():
            landed[:, face] = jnp.zeros((2, mode, load_width), jnp.float32)
            landed_half[:, face] = jnp.zeros((2, mode, load_width), jnp.bfloat16)

    def message(step, route):
        face, spot, _, target = route
        source = (
            initial.at[pl.ds(face * mode, mode)],
            sent.at[face],
            sent_half.at[0, face],
            sent_half.at[1, face],
        )[step]
        place = landed.at[step, spot] if step < 2 else landed_half.at[step - 2, spot]
        return pltpu.make_async_remote_copy(
            src_ref=source,
            dst_ref=place,
            send_sem=send_sems.at[0],
            recv_sem=recv_sems.at[step],
            device_id=target,
            device_id_type=pl.DeviceIdType.MESH,
        )

    def send(step, faces):
        for route in routes:
            if route[0] in faces:

                @pl.when(route[2])
                def _():
                    message(step, route).start()

    def wait_bytes(place, per_face, sem):
        for number in range(1, LINKED + 1):

            @pl.when(partners == number)
            def _():
                part = place.at[pl.ds(0, number * per_face)]
                pltpu.make_async_copy(part, part, sem).wait()

    def wait_arrived(step):
        place = landed.at[step] if step < 2 else landed_half.at[step - 2]
        wait_bytes(place, 1, recv_sems.at[step])

    def wait_sent():
        wait_bytes(near, 3, send_sems.at[0])

    def there(face):
        return jnp.where(routes[face][2], 1.0, 0.0)

    def face_span(face):
        return pl.ds(face * mode, mode)

    def block_rows(index):
        return slice(index * block, (index + 1) * block)

    weights = sweep_weights()

    def product_of(index, slot):
        span = block_span(index)
        if index == 0 and slot == 0:
            value = 0.0
            for chunk in range(chunks):
                wait_for(inv.at[0, pl.ds(0, block * (2 if chunk == 0 else 1))], chunk_sems[chunk])
                if chunk == 0:
                    load_slot(2)
                inside = pl.ds(chunk * block, block)
                value = value + dot_nn(wide[span, inside], inv[slot, inside])
        else:
            live = jnp.where(counts[0, 0] > slot, 1.0, 0.0)
            for piece in range(inner_width // NW):
                inside = pl.ds(piece * NW, NW)
                value = dot_nn(wide[span, inner_span(slot)], inv[slot, :, inside]) * live
                products[span, pl.ds(slot * inner_width + piece * NW, NW)] = value.astype(jnp.bfloat16)
            return
        value = value * jnp.where(counts[0, 0] > slot, 1.0, 0.0)
        products[span, inner_span(slot)] = value.astype(jnp.bfloat16)

    def keep_condensed(index, other, value):
        span, place = block_span(index), block_span(other)
        value = stiff[span, place].astype(jnp.float32) - value
        a_high[span, place], a_low[span, place] = two_parts(value)

    def condense_first(slot):
        for other in range(blocks):
            place = block_span(other)
            value = dot_nt(products[block_span(0), inner_span(slot)], wide[place, inner_span(slot)])
            if slot > 0:
                value = value + total[:, place]
            if slot + 1 < slots:
                total[:, place] = value
            else:
                keep_condensed(0, other, value)

    def condense(index):
        for other in range(index, blocks):
            keep_condensed(index, other, dot_nt(products[block_span(index), :], wide[block_span(other), :]))

    def applied(index, source, depth):
        span = block_span(index)
        ones = pl.ds(0, load_width)
        both, rest = [], []
        if index < depth:
            after = pl.ds(index * block, (depth - index) * block)
            both.append(dot_nt(source[:, after], a_high[span, after]))
            rest.append(dot_nt(source[ones, after], a_low[span, after]))
        if index > 0:
            before = pl.ds(0, min(index, depth) * block)
            both.append(dot_nn(source[:, before], a_high[before, span]))
            rest.append(dot_nn(source[ones, before], a_low[before, span]))
        both, rest = sum(both[1:], both[0]), sum(rest[1:], rest[0])
        return both[:load_width] + both[load_width:] + rest

    def keep_face_parts(place, span, value):
        high, low = two_parts(value)
        place[pl.ds(0, load_width), span] = high
        place[pl.ds(load_width, load_width), span] = low

    def keep_parts(value):
        high, low = two_parts(value)
        parts[pl.ds(0, load_width)] = high
        parts[pl.ds(load_width, load_width)] = low

    for slot in range(slots):
        if slot > 0:
            wait_slot(slot)
        if slot + 1 == slots:
            wait_for(stiff.at[pl.ds(0, (trace_width + block) // 2)], stiff_sem)
        product_of(0, slot)
        if slot == MEET:
            pl.semaphore_wait(barrier, partners)
            send(0, range(LINKED))
        if slot == 0:
            wait_for(wide.at[pl.ds(0, trace_width - block), inner_span(0)], rest_sem)
            wait_for(given, given_sem)
            load_slot(3)
            load_stiff()
        if slot < EARLY:
            product_of(1, slot)
        if slot == 0:
            start = given[0].T
            traces[...] = start
            keep_parts(start)
            bound_t[...] = given[1].T
        condense_first(slot)

    linked_blocks = LINKED // BLOCK_FACES
    for index in range(blocks):
        if index > 0:
            for slot in range(EARLY if index == 1 else 0, slots):
                product_of(index, slot)
            condense(index)
        span = block_span(index)
        value = bound_t[:, span] - applied(index, parts, blocks) - penalty_weight * traces[:, span]
        if index < linked_blocks:
            local[:, span] = value
            faces = range(index * BLOCK_FACES, (index + 1) * BLOCK_FACES)
            for face in faces:
                sent[face] = value[:, (face % BLOCK_FACES) * mode : (face % BLOCK_FACES + 1) * mode]
            send(1, faces)
        else:
            residual[:, span] = value
            change = weights[0][1] * value
            direction[:, span] = change
            keep_face_parts(more_parts, span, change)
        if index + 1 == linked_blocks:
            wait_arrived(0)
            for face in range(LINKED):
                span = face_span(face)
                value = local[:, span] + penalty_weight * landed[0, face].T
                residual[:, span] = value
                change = weights[0][1] * value
                direction[:, span] = change
                keep_face_parts(more_parts, span, change)

    for index in range(blocks):
        span = block_span(index)
        value = residual[:, span] - applied(index, more_parts, blocks) - penalty_weight * direction[:, span]
        local[:, span] = value
        faces = [face for face in range(LINKED) if face // BLOCK_FACES == index]
        for face in faces:
            sent_half[0, face] = value[
                :, (face % BLOCK_FACES) * mode : (face % BLOCK_FACES + 1) * mode
            ].astype(jnp.bfloat16)
        if index + 1 == linked_blocks:
            send(2, range(LINKED))

    wait_arrived(1)
    for face in range(FACES):
        span = face_span(face)
        value = local[:, span]
        if face < LINKED:
            beyond = (weights[0][1] * there(face)) * (landed[1, face] + penalty_weight * traces[:, span])
            near[face] = beyond
            value = value + penalty_weight * beyond
        change = weights[1][0] * direction[:, span] + weights[1][1] * value
        residual[:, span] = value
        near[FACES + face] = change
        keep_face_parts(parts, span, change)

    for index in range(blocks):
        value = applied(index, parts, blocks)
        for face in range(index * BLOCK_FACES, (index + 1) * BLOCK_FACES):
            span = face_span(face)
            lane = (face % BLOCK_FACES) * mode
            mine = residual[:, span] - value[:, lane : lane + mode] - penalty_weight * near[FACES + face]
            local[:, span] = mine
            if face < LINKED:
                view = sent_half[0, face].astype(jnp.float32) + penalty_weight * near[face]
                view_change = weights[1][0] * direction[:, span] + weights[1][1] * view
                sent_half[1, face] = (mine - (view - guess_slope * view_change)).astype(jnp.bfloat16)
        send(3, [face for face in range(LINKED) if face // BLOCK_FACES == index])
    for face in range(FACES):
        span = face_span(face)
        change = weights[2][0] * near[FACES + face] + weights[2][1] * local[:, span]
        keep_face_parts(more_parts, span, change)
        residual[:, span] = local[:, span] - penalty_weight * change
        traces[:, span] = traces[:, span] + direction[:, span] + near[FACES + face] + change
    for index in range(blocks):
        span = block_span(index)
        residual[:, span] = residual[:, span] - applied(index, more_parts, blocks)
    for index in range(linked_blocks, blocks):
        span = block_span(index)
        traces_out[span] = traces[:, span].T

    wait_arrived(2)
    for face in range(LINKED):
        span = face_span(face)
        view = landed_half[0, face].astype(jnp.float32) + penalty_weight * direction[:, span]
        beyond = there(face) * (weights[1][0] * near[face] + weights[1][1] * view)
        near[face] = beyond
        change = (weights[2][1] * penalty_weight) * beyond
        local[:, span] = change
        keep_face_parts(parts, span, change)

    for index in range(blocks):
        span = block_span(index)
        value = residual[:, span] - applied(index, parts, linked_blocks)
        if index < linked_blocks:
            for face in range(index * BLOCK_FACES, (index + 1) * BLOCK_FACES):
                lane = (face % BLOCK_FACES) * mode
                change = local[:, face_span(face)]
                mine = value[:, lane : lane + mode] + penalty_weight * (near[face] - change)
                residual_out[face_span(face)] = mine.T
                traces_out[face_span(face)] = (traces[:, face_span(face)] + change).T
        else:
            residual_out[span] = value.T
    for face in range(LINKED):
        span = face_span(face)
        view = landed_half[0, face].astype(jnp.float32) + penalty_weight * direction[:, span]
        landed[1, face] = view - guess_slope * near[face] + penalty_weight * near[FACES + face]

    wait_sent()
    wait_arrived(3)
    for face in range(LINKED):
        span = face_span(face)
        view = landed[1, face] + landed_half[1, face].astype(jnp.float32)
        beyond = weights[2][0] * near[face] + weights[2][1] * view
        beyond = (penalty_weight * there(face)) * beyond
        residual_out[span] = residual_out[span] + beyond.T


def write_kernel(traces, residual, traces_out, residual_out, sems):
    copies = [
        pltpu.make_async_copy(traces, traces_out, sems.at[0]),
        pltpu.make_async_copy(residual, residual_out, sems.at[1]),
    ]
    for copy in copies:
        copy.start()
    for copy in copies:
        copy.wait()


def in_hbm(value):
    return pltpu.with_memory_space_constraint(value, pltpu.HBM)


def on_device(
    axis_sizes, coupling, interior_inverse, boundary_stiffness, block_counts, initial_traces, trace_loads
):
    slots, trace_width, inner_width = coupling.shape[2:]
    load_width = initial_traces.shape[-1]
    mode = trace_width // FACES
    whole = pl.BlockSpec(memory_space=pltpu.HBM)
    vmem = pl.BlockSpec(memory_space=pltpu.VMEM)
    out = pltpu.VMEM((trace_width, load_width), jnp.float32)
    flat = pltpu.VMEM((load_width, trace_width), jnp.float32)
    square = pltpu.VMEM((trace_width, trace_width), jnp.bfloat16)
    long = pltpu.VMEM((trace_width, slots * inner_width), jnp.bfloat16)
    traces, residual = pl.pallas_call(
        functools.partial(kernel, axis_sizes),
        out_shape=(out, out),
        in_specs=[whole, whole, whole, pl.BlockSpec(memory_space=pltpu.SMEM), whole, whole],
        out_specs=(vmem, vmem),
        scratch_shapes=[
            long,
            pltpu.VMEM((slots, inner_width, inner_width), jnp.bfloat16),
            square,
            long,
            square,
            square,
            pltpu.VMEM((2, trace_width, load_width), jnp.float32),
            pltpu.VMEM((2 * load_width, trace_width), jnp.bfloat16),
            pltpu.VMEM((2 * load_width, trace_width), jnp.bfloat16),
            flat,
            flat,
            flat,
            flat,
            flat,
            pltpu.VMEM((2 * FACES, load_width, mode), jnp.float32),
            pltpu.VMEM((LINKED, load_width, mode), jnp.float32),
            pltpu.VMEM((2, LINKED, load_width, mode), jnp.bfloat16),
            pltpu.VMEM((2, LINKED, load_width, mode), jnp.float32),
            pltpu.VMEM((2, LINKED, load_width, mode), jnp.bfloat16),
            pltpu.VMEM((BLOCK_FACES * mode, trace_width), jnp.float32),
            pltpu.SemaphoreType.DMA((slots + 2 + inner_width * FACES // (BLOCK_FACES * trace_width),)),
            pltpu.SemaphoreType.DMA((1,)),
            pltpu.SemaphoreType.DMA((SWEEPS + 1,)),
        ],
        compiler_params=pltpu.CompilerParams(
            collective_id=0, has_side_effects=True, vmem_limit_bytes=48 << 20
        ),
        name="condense_and_sweep",
    )(
        in_hbm(coupling[0, 0]),
        in_hbm(interior_inverse[0, 0]),
        in_hbm(boundary_stiffness[0, 0]),
        block_counts,
        in_hbm(initial_traces[0, 0]),
        in_hbm(trace_loads[0, 0]),
    )
    result = jax.ShapeDtypeStruct((trace_width, load_width), jnp.float32)
    traces, residual = pl.pallas_call(
        write_kernel,
        out_shape=(result, result),
        in_specs=[vmem, vmem],
        out_specs=(whole, whole),
        scratch_shapes=[pltpu.SemaphoreType.DMA((2,))],
        name="write_results",
    )(
        pltpu.with_memory_space_constraint(traces, pltpu.VMEM),
        pltpu.with_memory_space_constraint(residual, pltpu.VMEM),
    )
    return (traces[None, None], residual[None, None])


def solution(mesh):
    in_specs = (
        P("gx", ("gy", "ha"), None, None, None),
        P("gx", ("gy", "ha"), None, None, None),
        P("gx", ("gy", "ha"), None, None),
        P("gx", ("gy", "ha")),
        P("gx", ("gy", "ha"), None, None),
        P("gx", ("gy", "ha"), None, None),
    )
    out_specs = (P("gx", ("gy", "ha"), None, None), P("gx", ("gy", "ha"), None, None))
    axis_sizes = (mesh.shape["gx"], mesh.shape["gy"], mesh.shape["ha"])
    return jax.shard_map(
        functools.partial(on_device, axis_sizes),
        mesh=mesh, in_specs=in_specs, out_specs=out_specs, check_vma=False,
    )
```
